8 devices in a mesh: dp: 2 (over z, y), cp: 4 (over x, core).
Axes of the slice: x: 2, y: 2, z: 1, core: 2. Of those that a mesh axis runs over, the one named last changes fastest.
Arguments:
- vis_feat: bfloat16 [16, 4096, 1152], P(('dp', 'cp')), parts along dimension 0
- text_emb: bfloat16 [8192, 2560], P(('dp', 'cp')), parts along dimension 0
- img_pos: int32 [16], P('dp'), parts along dimension 0
- grad_y: bfloat16 [8192, 2560], P(('dp', 'cp')), parts along dimension 0
- pn_gain: bfloat16 [1152], replicated
- w_proj: bfloat16 [1152, 2560], replicated
- pre_gain: bfloat16 [2560], replicated
- w_query: bfloat16 [2560, 2048], replicated
- w_key: bfloat16 [2560, 1024], replicated
- w_value: bfloat16 [2560, 1024], replicated
- q_gain: bfloat16 [256], replicated
- k_gain: bfloat16 [256], replicated
- w_out: bfloat16 [2048, 2560], replicated
- post_gain: bfloat16 [2560], replicated
Outputs:
- output 1: bfloat16 [8192, 2560], P(('dp', 'cp')), parts along dimension 0
- output 2: bfloat16 [8192, 2560], P(('dp', 'cp')), parts along dimension 0
- output 3: bfloat16 [16, 4096, 1152], P(('dp', 'cp')), parts along dimension 0
- output 4: bfloat16 [2304], P('dp'), parts along dimension 0
- output 5: bfloat16 [2304, 2560], P('dp'), parts along dimension 0
- output 6: bfloat16 [5120], P('dp'), parts along dimension 0
- output 7: bfloat16 [5120, 2048], P('dp'), parts along dimension 0
- output 8: bfloat16 [5120, 1024], P('dp'), parts along dimension 0
- output 9: bfloat16 [5120, 1024], P('dp'), parts along dimension 0
- output 10: bfloat16 [512], P('dp'), parts along dimension 0
- output 11: bfloat16 [512], P('dp'), parts along dimension 0
- output 12: bfloat16 [4096, 2560], P('dp'), parts along dimension 0
- output 13: bfloat16 [5120], P('dp'), parts along dimension 0
There are 2 independent parts. The reference program is written for one: setup_inputs(seed, part) draws one part's arguments, and reference() takes and returns one part's arrays. A program takes and returns all parts, laid end to end along the dimension named above; an argument that names none is the same for every part.
All inputs are finite; a program needn't handle non-finite values.
Results may differ from the reference program's by a relative error of at most 0.02.
Values are sent between devices in bfloat16 or wider.
A program may use at most 1 GiB of HBM per device.

```python
import functools
import jax
import jax.numpy as jnp
from jax import lax

D = 2560
HEADS = 8
KV_HEADS = 4
HEAD = 256
DV = 1152
SEQ_DEV = 1024
IMG_DEV = 2
GROUP = 4
GRID = 64
POOL = 4
SEQ = SEQ_DEV * GROUP
N_IMG = IMG_DEV * GROUP
SIDE = GRID // POOL
BLOCK = SIDE * SIDE
EPS = 1e-6
ROPE_BASE = 1000000.0
ROPE_SCALE = 8.0
NEG_BIG = -1e30


def place_images(rng_key):
    gap_key, perm_key = jax.random.split(rng_key)
    first_start = SEQ_DEV - BLOCK // 2
    spare = SEQ - N_IMG * BLOCK - first_start
    raw_gap = jax.random.randint(gap_key, (N_IMG,), 0, 8)
    weight = raw_gap * raw_gap * raw_gap
    gap_total = jnp.maximum(jnp.sum(weight), 1)
    gap_rows = spare * weight // gap_total
    slot_start = first_start + jnp.arange(N_IMG) * BLOCK + jnp.cumsum(gap_rows) - gap_rows
    slot_order = jax.random.permutation(perm_key, N_IMG)
    return slot_start[slot_order].astype(jnp.int32)


def draw_normal(rng_key, arr_shape, std_scale):
    return (jax.random.normal(rng_key, arr_shape, jnp.float32) * std_scale).astype(jnp.bfloat16)


def setup_inputs(seed: int = 0, part: int = 0) -> dict:
    base_key = jax.random.key(seed)
    part_keys = jax.random.split(jax.random.fold_in(base_key, part), 4)
    weight_keys = jax.random.split(jax.random.key(seed + 1), 10)
    return {
        'vis_feat': draw_normal(part_keys[0], (N_IMG, GRID * GRID, DV), 1.0),
        'text_emb': draw_normal(part_keys[1], (SEQ, D), 1.0),
        'img_pos': place_images(part_keys[2]),
        'grad_y': draw_normal(part_keys[3], (SEQ, D), 1.0),
        'pn_gain': draw_normal(weight_keys[0], (DV,), 0.3),
        'w_proj': draw_normal(weight_keys[1], (DV, D), DV ** -0.5),
        'pre_gain': draw_normal(weight_keys[2], (D,), 0.3),
        'w_query': draw_normal(weight_keys[3], (D, HEADS * HEAD), D ** -0.5),
        'w_key': draw_normal(weight_keys[4], (D, KV_HEADS * HEAD), D ** -0.5),
        'w_value': draw_normal(weight_keys[5], (D, KV_HEADS * HEAD), D ** -0.5),
        'q_gain': draw_normal(weight_keys[6], (HEAD,), 0.3),
        'k_gain': draw_normal(weight_keys[7], (HEAD,), 0.3),
        'w_out': draw_normal(weight_keys[8], (HEADS * HEAD, D), (HEADS * HEAD) ** -0.5),
        'post_gain': draw_normal(weight_keys[9], (D,), 0.3),
    }


def rms_scale(values, gain_vec):
    wide_vals = values.astype(jnp.float32)
    mean_sq = jnp.mean(wide_vals * wide_vals, axis=-1, keepdims=True)
    return wide_vals * lax.rsqrt(mean_sq + EPS) * (1.0 + gain_vec.astype(jnp.float32))


def rope_tables(positions):
    inv_freq = ROPE_BASE ** (-jnp.arange(0, HEAD, 2).astype(jnp.float32) / HEAD)
    rot_angle = (positions.astype(jnp.float32) / ROPE_SCALE)[:, None] * inv_freq[None, :]
    rot_angle = jnp.concatenate([rot_angle, rot_angle], axis=-1)
    return jnp.cos(rot_angle)[:, None, :], jnp.sin(rot_angle)[:, None, :]


def apply_rope(values, cos_t, sin_t):
    half_dim = values.shape[-1] // 2
    rotated = jnp.concatenate([-values[..., half_dim:], values[..., :half_dim]], axis=-1)
    return values * cos_t + rotated * sin_t


def project(vis_feat, pn_gain, w_proj):
    img_count = vis_feat.shape[0]
    patch_grid = vis_feat.reshape(img_count, SIDE, POOL, SIDE, POOL, DV).astype(jnp.float32)
    pooled = (jnp.sum(patch_grid, axis=(2, 4)) / (POOL * POOL)).astype(jnp.bfloat16)
    normed = rms_scale(pooled.reshape(img_count * BLOCK, DV), pn_gain).astype(jnp.bfloat16)
    return jnp.dot(normed, w_proj, preferred_element_type=jnp.float32).astype(jnp.bfloat16)


def attend_block(q_blk, start_blk, blk_index, k_heads, v_heads):
    groups = HEADS // KV_HEADS
    q_pos = blk_index * SEQ_DEV + jnp.arange(SEQ_DEV)
    key_pos = jnp.arange(SEQ)
    in_image = (start_blk[:, None] >= 0) & (key_pos[None, :] >= start_blk[:, None]) & (key_pos[None, :] < start_blk[:, None] + BLOCK)
    visible = (key_pos[None, :] <= q_pos[:, None]) | in_image
    q_grp = q_blk.reshape(SEQ_DEV, KV_HEADS, groups, HEAD).astype(jnp.float32)
    scores = jnp.einsum('qkgd,skd->kgqs', q_grp, k_heads.astype(jnp.float32)) * HEAD ** -0.5
    scores = jnp.where(visible[None, None], scores, NEG_BIG)
    prob_lo = jax.nn.softmax(scores, axis=-1).astype(jnp.bfloat16)
    attn_blk = jnp.einsum('kgqs,skd->qkgd', prob_lo.astype(jnp.float32), v_heads.astype(jnp.float32))
    return attn_blk.astype(jnp.bfloat16).reshape(SEQ_DEV, HEADS * HEAD)


def forward(vis_feat, text_emb, pn_gain, w_proj, pre_gain, w_query, w_key, w_value, q_gain, k_gain, w_out, post_gain, img_pos):
    soft_tok = project(vis_feat, pn_gain, w_proj)
    img_rows = (img_pos[:, None] + jnp.arange(BLOCK)[None, :]).reshape(-1)
    merged = text_emb.at[img_rows].set(soft_tok)
    starts = jnp.full((SEQ,), -1, jnp.int32).at[img_rows].set(jnp.repeat(img_pos, BLOCK))
    hidden = rms_scale(merged, pre_gain).astype(jnp.bfloat16)
    q_raw = jnp.dot(hidden, w_query, preferred_element_type=jnp.float32).astype(jnp.bfloat16).reshape(SEQ, HEADS, HEAD)
    k_raw = jnp.dot(hidden, w_key, preferred_element_type=jnp.float32).astype(jnp.bfloat16).reshape(SEQ, KV_HEADS, HEAD)
    v_heads = jnp.dot(hidden, w_value, preferred_element_type=jnp.float32).astype(jnp.bfloat16).reshape(SEQ, KV_HEADS, HEAD)
    cos_t, sin_t = rope_tables(jnp.arange(SEQ))
    q_heads = apply_rope(rms_scale(q_raw, q_gain), cos_t, sin_t).astype(jnp.bfloat16)
    k_heads = apply_rope(rms_scale(k_raw, k_gain), cos_t, sin_t).astype(jnp.bfloat16)
    block_fn = jax.checkpoint(attend_block)
    attn_out = lax.map(lambda blk_args: block_fn(blk_args[0], blk_args[1], blk_args[2], k_heads, v_heads), (q_heads.reshape(GROUP, SEQ_DEV, HEADS, HEAD), starts.reshape(GROUP, SEQ_DEV), jnp.arange(GROUP)))
    attn_out = attn_out.reshape(SEQ, HEADS * HEAD)
    proj_out = jnp.dot(attn_out, w_out, preferred_element_type=jnp.float32).astype(jnp.bfloat16)
    return (merged.astype(jnp.float32) + rms_scale(proj_out, post_gain)).astype(jnp.bfloat16)


def reference(vis_feat, text_emb, img_pos, grad_y, pn_gain, w_proj, pre_gain, w_query, w_key, w_value, q_gain, k_gain, w_out, post_gain):
    y_out, pullback = jax.vjp(functools.partial(forward, img_pos=img_pos), vis_feat, text_emb, pn_gain, w_proj, pre_gain, w_query, w_key, w_value, q_gain, k_gain, w_out, post_gain)
    grad_list = pullback(grad_y)
    return (y_out, grad_list[1], grad_list[0], grad_list[2], grad_list[3], grad_list[4], grad_list[5], grad_list[6], grad_list[7], grad_list[8], grad_list[9], grad_list[10], grad_list[11])
```

```python
import functools
import jax
import jax.numpy as jnp
from jax import lax
from jax.experimental import pallas as pl
from jax.experimental.pallas import tpu as pltpu
from jax.sharding import PartitionSpec as P

GRID = 64
POOL = 4
SIDE = GRID // POOL
BLK = SIDE * SIDE
HD = 256
HD2 = 2 * HD
ROWS = 1024
CHIP = 2 * ROWS
SEQ = 2 * CHIP
LANES = 128
YES = True
ALL = ...
ONE = 1.0
EPS = 1e-6
ROPE_BASE = 1000000.0
ROPE_SCALE = 8.0
NEG_BIG = -1e30
LOG2E = 1.4426950408889634
BF = jnp.bfloat16
F32 = jnp.float32
FAR = 1 << 20
VMEM_MAX = 67043328

XPERM = [(0, 2), (2, 0), (1, 3), (3, 1)]
SPERM = [(0, 1), (1, 0), (2, 3), (3, 2)]


def dot(a, b):
    return lax.dot_general(a, b, (((1,), (0,)), ((), ())), preferred_element_type=F32)


def dot_nt(a, b):
    return lax.dot_general(a, b, (((1,), (1,)), ((), ())), preferred_element_type=F32)


def dot_tn(a, b):
    return lax.dot_general(a, b, (((0,), (0,)), ((), ())), preferred_element_type=F32)


def params(n_grid, **kw):
    return pltpu.CompilerParams(dimension_semantics=("arbitrary",) * n_grid, vmem_limit_bytes=kw.pop("vmem", VMEM_MAX - (1 << 20)), **kw)


def cost(flops, nbytes):
    return pl.CostEstimate(flops=int(flops), bytes_accessed=int(nbytes), transcendentals=0)


def const_spec(shape):
    return pl.BlockSpec(shape, lambda *a: (0,) * len(shape), pipeline_mode=pl.Buffered(1))


ANY = pl.BlockSpec(memory_space=pl.ANY)


def pool_kernel(vis_ref, gain_ref, pooled_ref, normed_ref):
    row = lax.broadcasted_iota(jnp.int32, (GRID, ROWS), 0)
    src = lax.broadcasted_iota(jnp.int32, (GRID, ROWS), 1)
    hit = (row // SIDE == src // HD) & (row % SIDE == (src % GRID) // POOL)
    mask = jnp.where(hit, ONE, 0.0).astype(BF)
    pooled = (dot(mask, vis_ref[0]) * (ONE / 16.0)).astype(BF)
    pooled_ref[ALL] = pooled
    wide = pooled.astype(F32)
    rs = lax.rsqrt(jnp.mean(wide * wide, axis=1, keepdims=YES) + EPS)
    normed_ref[ALL] = (wide * rs * (ONE + gain_ref[ALL])).astype(BF)


def pool_call(vis, gain):
    n, _, dv = vis.shape
    return pl.pallas_call(
        pool_kernel,
        grid=(n * POOL,),
        in_specs=[pl.BlockSpec((1, ROWS, dv), lambda i: (i // POOL, i % POOL, 0)), const_spec((1, dv))],
        out_specs=[pl.BlockSpec((GRID, dv), lambda i: (i, 0))] * 2,
        out_shape=[jax.ShapeDtypeStruct((n * BLK, dv), BF)] * 2,
        compiler_params=params(1),
        cost_estimate=cost(2 * HD2 * ROWS * dv, vis.size * 2),
        name="pool",
    )(vis, gain)


def merge_kernel(tab, sc, soft, text, gain, x_ref, h_ref):
    b = sc[0] * POOL + pl.program_id(0)
    ia, da, ib, db = tab[POOL * b], tab[POOL * b + 1], tab[POOL * b + 2], tab[POOL * b + 3]
    some = (da < FAR) | (db < FAR)

    @pl.when(some)
    def _():
        row = lax.broadcasted_iota(jnp.int32, (HD, HD), 0)
        col = lax.broadcasted_iota(jnp.int32, (HD, HD), 1)
        pa = jnp.where(col == row + da, ONE, 0.0).astype(BF)
        pb = jnp.where(col == row + db, ONE, 0.0).astype(BF)
        sa = soft[pl.ds(pl.multiple_of(ia * HD, HD), HD), :]
        sb = soft[pl.ds(pl.multiple_of(ib * HD, HD), HD), :]
        val = (dot(pa, sa) + dot(pb, sb)).astype(BF)
        r1 = lax.broadcasted_iota(jnp.int32, (HD, 1), 0)
        ina = (r1 + da >= 0) & (r1 + da < HD)
        inb = (r1 + db >= 0) & (r1 + db < HD)
        x_ref[ALL] = jnp.where(ina | inb, val, text[ALL])

    @pl.when(jnp.logical_not(some))
    def _():
        x_ref[ALL] = text[ALL]

    xv = x_ref[ALL].astype(F32)
    rs = lax.rsqrt(jnp.mean(xv * xv, axis=1, keepdims=YES) + EPS)
    h_ref[ALL] = (xv * rs * (ONE + gain[ALL])).astype(BF)


def merge_call(tab, rr, soft, text, gain):
    rows, d = text.shape
    spec = pl.BlockSpec((HD, d), lambda i, *_: (i, 0))
    return pl.pallas_call(
        merge_kernel,
        grid_spec=pltpu.PrefetchScalarGridSpec(
            num_scalar_prefetch=2,
            grid=(rows // HD,),
            in_specs=[const_spec(soft.shape), spec, const_spec((1, d))],
            out_specs=[spec, spec],
        ),
        out_shape=[jax.ShapeDtypeStruct((rows, d), BF)] * 2,
        compiler_params=params(1),
        cost_estimate=cost(2 * rows * HD2 * d, (rows * 3 + soft.shape[0]) * d * 2),
        name="merge",
    )(tab, rr, soft, text, gain)


def rope_fwd(raw, gain, cos, sin):
    rs = lax.rsqrt(jnp.mean(raw * raw, axis=1, keepdims=YES) + EPS)
    n = raw * rs * (ONE + gain)
    a, b = n[:, :LANES], n[:, LANES:]
    return jnp.concatenate([a * cos - b * sin, b * cos + a * sin], axis=1)


def qkv_kernel(sc, ha, hb, wq, wk, wv, qg, kg, cos_ref, sin_ref, *rest):
    outs = rest[-10:]
    q_o, qr_o, k_o, kr_o, v_o = outs[0:2], outs[2:POOL], outs[POOL:6], outs[6:8], outs[8:10]
    hid = jnp.where(pl.program_id(0) < 2, ha[ALL], hb[ALL])
    cos, sin = cos_ref[ALL], sin_ref[ALL]
    for g in range(2):
        aq = dot(hid, wq[:, HD2 * g : HD2 * g + HD2]).astype(BF)
        qr_o[g][ALL] = aq
        for h in range(2):
            raw = aq[:, HD * h : HD * h + HD].astype(F32)
            q_o[g][:, HD * h : HD * h + HD] = (rope_fwd(raw, qg[ALL], cos, sin) * 0.0625).astype(BF)
        ak = dot(hid, wk[:, HD * g : HD * g + HD]).astype(BF)
        kr_o[g][ALL] = ak
        k_o[g][ALL] = rope_fwd(ak.astype(F32), kg[ALL], cos, sin).astype(BF)
        v_o[g][ALL] = dot(hid, wv[:, HD * g : HD * g + HD]).astype(BF)


def qkv_call(sc, ha, hb, wq, wk, wv, qg, kg, cos, sin, bufs):
    d = ha.shape[1]
    rows = HD2

    def outrow(i, s):
        return s[0] * POOL + jnp.where(i < 2, s[1] * 2 + i, (1 - s[1]) * 2 + i - 2)

    def ospec(w):
        return pl.BlockSpec((rows, w), lambda i, s: (outrow(i, s), 0))

    one = dict(pipeline_mode=pl.Buffered(1))
    widths = [HD2, HD2, HD2, HD2, HD, HD, HD, HD, HD, HD]
    in_specs = [
        pl.BlockSpec((rows, d), lambda i, s: (jnp.minimum(i, 1), 0)),
        pl.BlockSpec((rows, d), lambda i, s: (jnp.maximum(i - 2, 0), 0)),
        pl.BlockSpec((d, ROWS), lambda i, s: (0, s[1]), **one),
        pl.BlockSpec((d, HD2), lambda i, s: (0, s[1]), **one),
        pl.BlockSpec((d, HD2), lambda i, s: (0, s[1]), **one),
        const_spec((1, HD)),
        const_spec((1, HD)),
        ospec(LANES),
        ospec(LANES),
    ]
    args = [sc, ha, hb, wq, wk, wv, qg, kg, cos, sin]
    alias = {}
    if bufs is not None:
        alias = {len(args) + n: n for n in range(10)}
        in_specs += [ANY] * 10
        args += list(bufs)
    seq = POOL * ha.shape[0]
    return pl.pallas_call(
        qkv_kernel,
        grid_spec=pltpu.PrefetchScalarGridSpec(
            num_scalar_prefetch=1, grid=(POOL,), in_specs=in_specs, out_specs=[ospec(w) for w in widths]
        ),
        out_shape=[jax.ShapeDtypeStruct((seq, w), BF) for w in widths],
        input_output_aliases=alias,
        compiler_params=params(1),
        cost_estimate=cost(2 * CHIP * d * CHIP, CHIP * (d + 3584) * 2 + d * CHIP * 2),
        name="qkv",
    )(*args)


QB = 512
KB = 512


def fwd_kernel(nkv, q_ref, k_ref, v_ref, bs_ref, o_ref, lse_ref, m_s, l_s, acc_s):
    i = pl.program_id(0)
    m_s[ALL] = jnp.full(m_s.shape, NEG_BIG, F32)
    l_s[ALL] = jnp.zeros(l_s.shape, F32)
    acc_s[ALL] = jnp.zeros(acc_s.shape, F32)

    def step(j, masked):
        off = pl.multiple_of(j * KB, KB)
        kb = k_ref[pl.ds(off, KB), :]
        vb = v_ref[pl.ds(off, KB), :]
        if masked:
            qpos = i * QB + lax.broadcasted_iota(jnp.int32, (QB, KB), 0)
            kpos = j * KB + lax.broadcasted_iota(jnp.int32, (QB, KB), 1)
            rel = kpos - bs_ref[ALL]
            vis = (kpos <= qpos) | ((rel >= 0) & (rel < BLK))
        ss = [dot_nt(q_ref[:, HD * h : HD * h + HD], kb) for h in range(2)]
        for h in range(2):
            s = ss[h]
            if masked:
                s = jnp.where(vis, s, NEG_BIG)
            parts = [s[:, LANES * t : LANES * t + LANES] for t in range(KB // LANES)]
            mx = functools.reduce(jnp.maximum, parts)
            mx = jnp.broadcast_to(jnp.max(mx, axis=1, keepdims=YES), (QB, LANES))
            m_old = m_s[h]
            m_new = jnp.maximum(m_old, mx)
            alpha = jnp.exp2((m_old - m_new) * LOG2E)
            ps = [jnp.exp2((t - m_new) * LOG2E) for t in parts]
            l_s[h] = l_s[h] * alpha + functools.reduce(jnp.add, ps)
            m_s[h] = m_new
            p = jnp.concatenate([t.astype(BF) for t in ps], axis=1)
            acc_s[h] = acc_s[h] * jnp.concatenate([alpha, alpha], axis=1) + dot(p, vb)

    lax.fori_loop(0, i, lambda j, c: (step(j, False), c)[1], 0)
    step(i, YES)

    @pl.when(nkv[i] > i + 1)
    def _():
        step(i + 1, YES)

    for h in range(2):
        l = jnp.broadcast_to(jnp.sum(l_s[h], axis=1, keepdims=YES), (QB, LANES))
        inv = ONE / l
        o_ref[:, HD * h : HD * h + HD] = (acc_s[h] * jnp.concatenate([inv, inv], axis=1)).astype(BF)
        lse = m_s[h] * LOG2E + jnp.log2(l)
        lse_ref[0, h : h + 1, :] = jnp.transpose(lse)[0:1, :]


def fwd_call(nkv, q, k, v, bs_col):
    seq = q.shape[0]
    n = seq // QB
    return pl.pallas_call(
        fwd_kernel,
        grid_spec=pltpu.PrefetchScalarGridSpec(
            num_scalar_prefetch=1,
            grid=(n,),
            in_specs=[
                pl.BlockSpec((QB, HD2), lambda i, *_: (i, 0)),
                const_spec((seq, HD)),
                const_spec((seq, HD)),
                pl.BlockSpec((QB, 1), lambda i, *_: (i, 0)),
            ],
            out_specs=[pl.BlockSpec((QB, HD2), lambda i, *_: (i, 0)), pl.BlockSpec((1, 2, QB), lambda i, *_: (i, 0, 0))],
            scratch_shapes=[pltpu.VMEM((2, QB, LANES), F32), pltpu.VMEM((2, QB, LANES), F32), pltpu.VMEM((2, QB, HD), F32)],
        ),
        out_shape=[jax.ShapeDtypeStruct((seq, HD2), BF), jax.ShapeDtypeStruct((n, 2, QB), F32)],
        compiler_params=params(1),
        cost_estimate=cost(2 * 2 * 2 * seq * seq * HD * 0.7, seq * 1536 * 2),
        name="attn_fwd",
    )(nkv, q, k, v, bs_col)


def out_kernel(sc, oo0, oo1, os0, os1, wo, x_ref, dy_ref, gain, *rest):
    y_ref = rest[0] if len(rest) == 7 else None
    dp_ref, da_o0, da_o1, da_s0, da_s1, gp_ref = rest[-6:]
    c = sc[1]
    own = pl.multiple_of(c * ROWS, ROWS)
    sib = pl.multiple_of((1 - c) * ROWS, ROWS)
    a = dot(oo0[ALL], wo[pl.ds(own, HD2), :])
    a = a + dot(oo1[ALL], wo[pl.ds(own + HD2, HD2), :])
    a = a + dot(os0[ALL], wo[pl.ds(sib, HD2), :])
    a = a + dot(os1[ALL], wo[pl.ds(sib + HD2, HD2), :])
    a = a.astype(BF).astype(F32)
    rs = lax.rsqrt(jnp.mean(a * a, axis=1, keepdims=YES) + EPS)
    g1 = ONE + gain[ALL]
    n = a * rs
    if y_ref is not None:
        y_ref[ALL] = (x_ref[ALL].astype(F32) + n * g1).astype(BF)
    dy = dy_ref[ALL].astype(F32)
    dyn = dy * n

    @pl.when(pl.program_id(0) == 0)
    def _():
        gp_ref[ALL] = jnp.zeros_like(gp_ref)

    gp_ref[ALL] += jnp.sum(dyn, axis=0, keepdims=YES)
    mean = jnp.mean(dyn * g1, axis=1, keepdims=YES)
    dp = ((dy * g1 - n * mean) * rs).astype(BF)
    dp_ref[ALL] = dp
    da_o0[ALL] = dot_nt(dp, wo[pl.ds(own, HD2), :]).astype(BF)
    da_o1[ALL] = dot_nt(dp, wo[pl.ds(own + HD2, HD2), :]).astype(BF)
    da_s0[ALL] = dot_nt(dp, wo[pl.ds(sib, HD2), :]).astype(BF)
    da_s1[ALL] = dot_nt(dp, wo[pl.ds(sib + HD2, HD2), :]).astype(BF)


def out_call(sc, oo, osib, wo, x, dy, gain, want_y):
    rows, d = dy.shape
    rb = HD
    nb = rows // rb

    def orow(i, s):
        return (s[0] * 2 + s[1]) * nb + i

    ospec = pl.BlockSpec((rb, HD2), lambda i, s: (orow(i, s), 0))
    rspec = pl.BlockSpec((rb, d), lambda i, s: (i, 0))
    pspec = pl.BlockSpec((rb, HD2), lambda i, s: (i, 0))
    out_specs = [rspec] * (2 if want_y else 1) + [pspec] * POOL + [pl.BlockSpec((1, d), lambda i, s: (0, 0))]
    out_shape = (
        [jax.ShapeDtypeStruct((rows, d), BF)] * (2 if want_y else 1)
        + [jax.ShapeDtypeStruct((rows, HD2), BF)] * POOL
        + [jax.ShapeDtypeStruct((1, d), F32)]
    )
    return pl.pallas_call(
        out_kernel,
        grid_spec=pltpu.PrefetchScalarGridSpec(
            num_scalar_prefetch=1,
            grid=(nb,),
            in_specs=[ospec] * POOL + [const_spec(wo.shape), rspec, rspec, const_spec((1, d))],
            out_specs=out_specs,
        ),
        out_shape=out_shape,
        compiler_params=params(1),
        cost_estimate=cost(POOL * rows * d * CHIP, rows * d * 2 * 5 + wo.size * 2),
        name="out_proj",
    )(sc, oo[0], oo[1], osib[0], osib[1], wo, x, dy, gain)


def rope_norm_bwd(dy, raw, gain, cos, sin):
    d1, d2 = dy[:, :LANES], dy[:, LANES:]
    dn = jnp.concatenate([d1 * cos + d2 * sin, d2 * cos - d1 * sin], axis=1)
    rs = lax.rsqrt(jnp.mean(raw * raw, axis=1, keepdims=YES) + EPS)
    n = raw * rs
    dnn = dn * n
    gg = jnp.sum(dnn, axis=0, keepdims=YES)
    mean = jnp.mean(dnn * (ONE + gain), axis=1, keepdims=YES)
    return ((dn * (ONE + gain) - n * mean) * rs).astype(BF), gg


def bwd_kernel(
    sc, q_ref, dox, doy, o_ref, k_ref, v_ref, lse_ref, bs_ref, qr_ref, kr_ref, cos_ref, sin_ref, qg, kg,
    out_ref, gq_ref, gk_ref, do_s, dl_s, dq_s, dk_s, dv_s, sem,
):
    j = pl.program_id(0)
    nj = pl.num_programs(0)
    c = sc[0]

    @pl.when(j == 0)
    def _():
        cps = []
        for xx in range(2):
            for src, cc in ((dox, c), (doy, 1 - c)):
                dst = do_s.at[pl.ds(pl.multiple_of(xx * CHIP + cc * ROWS, ROWS), ROWS), :]
                cps.append(pltpu.make_async_copy(src.at[xx], dst, sem.at[len(cps)]))
        for cp in cps:
            cp.start()
        dq_s[ALL] = jnp.zeros_like(dq_s)
        gq_ref[ALL] = jnp.zeros_like(gq_ref)
        gk_ref[ALL] = jnp.zeros_like(gk_ref)
        for cp in cps:
            cp.wait()

        def delta(i, carry):
            off = pl.multiple_of(i * QB, QB)
            pr = do_s[pl.ds(off, QB), :].astype(F32) * o_ref[pl.ds(off, QB), :].astype(F32)
            for h in range(2):
                col = jnp.sum(pr[:, HD * h : HD * h + HD], axis=1, keepdims=YES)
                dl_s[i, h : h + 1, :] = jnp.transpose(jnp.broadcast_to(col, (QB, LANES)))[0:1, :]
            return carry

        lax.fori_loop(0, SEQ // QB, delta, 0)

    dk_s[ALL] = jnp.zeros_like(dk_s)
    dv_s[ALL] = jnp.zeros_like(dv_s)
    kb = k_ref[ALL]
    vb = v_ref[ALL]

    def step(i, masked):
        off = pl.multiple_of(i * QB, QB)
        if masked:
            kpos = j * KB + lax.broadcasted_iota(jnp.int32, (KB, QB), 0)
            qpos = i * QB + lax.broadcasted_iota(jnp.int32, (KB, QB), 1)
            rel = kpos - bs_ref[i]
            vis = (kpos <= qpos) | ((rel >= 0) & (rel < BLK))
        qs = [q_ref[pl.ds(off, QB), HD * h : HD * h + HD] for h in range(2)]
        dos = [do_s[pl.ds(off, QB), HD * h : HD * h + HD] for h in range(2)]
        st = [dot_nt(kb, qs[h]) for h in range(2)]
        dpt = [dot_nt(vb, dos[h]) for h in range(2)]
        for h in range(2):
            pt = jnp.exp2(st[h] * LOG2E - lse_ref[i, h : h + 1, :])
            if masked:
                pt = jnp.where(vis, pt, 0.0)
            dst = (pt * (dpt[h] - dl_s[i, h : h + 1, :])).astype(BF)
            dv_s[ALL] += dot(pt.astype(BF), dos[h])
            dk_s[ALL] += dot(dst, qs[h])
            dq_s[pl.ds(off, QB), HD * h : HD * h + HD] += dot_tn(dst, kb)

    @pl.when(sc[1 + j] < j)
    def _():
        step(jnp.maximum(j - 1, 0), YES)

    step(j, YES)
    lax.fori_loop(j + 1, nj, lambda i, cr: (step(i, False), cr)[1], 0)

    koff = pl.multiple_of(j * KB, KB)
    dk, gk = rope_norm_bwd(
        dk_s[ALL].astype(BF).astype(F32), kr_ref[ALL].astype(F32), kg[ALL], cos_ref[pl.ds(koff, KB), :], sin_ref[pl.ds(koff, KB), :]
    )
    gk_ref[ALL] += gk
    out_ref[pl.ds(koff, KB), HD2:768] = dk
    out_ref[pl.ds(koff, KB), 768:ROWS] = dv_s[ALL].astype(BF)

    @pl.when(j == nj - 1)
    def _():
        def fin(i, carry):
            off = pl.multiple_of(i * HD, HD)
            cos, sin = cos_ref[pl.ds(off, HD), :], sin_ref[pl.ds(off, HD), :]
            for h in range(2):
                sl = slice(HD * h, HD * h + HD)
                dq = (dq_s[pl.ds(off, HD), sl] * 0.0625).astype(BF).astype(F32)
                dqr, gq = rope_norm_bwd(dq, qr_ref[pl.ds(off, HD), sl].astype(F32), qg[ALL], cos, sin)
                gq_ref[ALL] += gq
                out_ref[pl.ds(off, HD), sl] = dqr
            return carry

        lax.fori_loop(0, SEQ // HD, fin, 0)


def bwd_call(sc, q, do_own, do_sib, o, k, v, lse, bs_row, qr, kr, cos, sin, qg, kg):
    seq = q.shape[0]
    nj = seq // KB
    return pl.pallas_call(
        bwd_kernel,
        grid_spec=pltpu.PrefetchScalarGridSpec(
            num_scalar_prefetch=1,
            grid=(nj,),
            in_specs=[
                const_spec((seq, HD2)),
                ANY,
                ANY,
                const_spec((seq, HD2)),
                pl.BlockSpec((KB, HD), lambda j, *_: (j, 0)),
                pl.BlockSpec((KB, HD), lambda j, *_: (j, 0)),
                const_spec(lse.shape),
                const_spec(bs_row.shape),
                const_spec((seq, HD2)),
                pl.BlockSpec((KB, HD), lambda j, *_: (j, 0)),
                const_spec((seq, LANES)),
                const_spec((seq, LANES)),
                const_spec((1, HD)),
                const_spec((1, HD)),
            ],
            out_specs=[
                pl.BlockSpec((seq, ROWS), lambda j, *_: (0, 0)),
                pl.BlockSpec((1, HD), lambda j, *_: (0, 0)),
                pl.BlockSpec((1, HD), lambda j, *_: (0, 0)),
            ],
            scratch_shapes=[
                pltpu.VMEM((seq, HD2), BF),
                pltpu.VMEM((seq // QB, 2, QB), F32),
                pltpu.VMEM((seq, HD2), F32),
                pltpu.VMEM((KB, HD), F32),
                pltpu.VMEM((KB, HD), F32),
                pltpu.SemaphoreType.DMA((POOL,)),
            ],
        ),
        out_shape=[
            jax.ShapeDtypeStruct((seq, ROWS), BF),
            jax.ShapeDtypeStruct((1, HD), F32),
            jax.ShapeDtypeStruct((1, HD), F32),
        ],
        compiler_params=params(1),
        cost_estimate=cost(5 * 2 * 2 * seq * seq * HD * 0.6, seq * 4000 * 2),
        name="attn_bwd",
    )(sc, q, do_own, do_sib, o, k, v, lse, bs_row, qr, kr, cos, sin, qg, kg)


def gwo_kernel(sc, o0, o1, dp0, dp1, dps0, dps1, out_ref, acc):
    s = pl.program_id(0)
    o = jnp.where(sc[0] == 0, o0[ALL], o1[ALL])

    @pl.when(s == 0)
    def _():
        acc[ALL] = jnp.zeros_like(acc)

    for n, ref in enumerate((dp0, dp1, dps0, dps1)):

        @pl.when(s // 2 == n)
        def _():
            acc[ALL] += dot_tn(o, ref[ALL])

    @pl.when(s == pl.num_programs(0) - 1)
    def _():
        out_ref[ALL] = acc[ALL].astype(BF)


def gwo_call(sc, o0, o1, dps):
    seq = o0.shape[0]
    d = dps[0].shape[1]

    def orow(s, p):
        n = s // 2
        core = jnp.where(n < 2, p[1], 1 - p[1])
        return ((n % 2) * 2 + core) * 2 + s % 2

    ospec = pl.BlockSpec((HD2, HD2), lambda s, p: (orow(s, p), 0))
    dspecs = [pl.BlockSpec((HD2, d), lambda s, p, n=n: (jnp.clip(s - 2 * n, 0, 1), 0)) for n in range(POOL)]
    return pl.pallas_call(
        gwo_kernel,
        grid_spec=pltpu.PrefetchScalarGridSpec(
            num_scalar_prefetch=1,
            grid=(8,),
            in_specs=[ospec, ospec] + dspecs,
            out_specs=pl.BlockSpec((HD2, d), lambda s, p: (0, 0)),
            scratch_shapes=[pltpu.VMEM((HD2, d), F32)],
        ),
        out_shape=jax.ShapeDtypeStruct((HD2, d), BF),
        compiler_params=params(1),
        cost_estimate=cost(2 * seq * HD2 * d, seq * (d + ROWS) * 2),
        name="grad_wo",
    )(sc, o0, o1, *dps)


def gqkv_kernel(sc, h0, h1, h2, h3, p0, p1, s0, s1, gq_ref, gk_ref, gv_ref, acc):
    k = pl.program_id(1)
    c = sc[1]

    @pl.when(k == 0)
    def _():
        acc[ALL] = jnp.zeros_like(acc)

    r = k // 2
    xr = r ^ sc[2]
    for n, ref in enumerate((h0, h1, h2, h3)):

        @pl.when(xr == n)
        def _():
            h = ref[ALL]
            for t, part in enumerate((p0, p1, s0, s1)):
                acc[:, ROWS * t : ROWS * t + ROWS] += dot_tn(h, part[ALL])

    @pl.when(k == pl.num_programs(1) - 1)
    def _():
        for t in range(POOL):
            cc = c if t < 2 else 1 - c
            g = t % 2
            base = ROWS * t
            gq_ref[:, pl.ds(pl.multiple_of(cc * ROWS + HD2 * g, HD2), HD2)] = acc[:, base : base + HD2].astype(BF)
            kv = pl.ds(pl.multiple_of(cc * HD2 + HD * g, HD), HD)
            gk_ref[:, kv] = acc[:, base + HD2 : base + 768].astype(BF)
            gv_ref[:, kv] = acc[:, base + 768 : base + ROWS].astype(BF)


def gqkv_call(sc, hids, parts):
    seq = parts[0].shape[0]
    half = hids[0].shape[1] // 2
    mrow = half // 2

    def hspec(n):
        def im(m, k, p):
            return (jnp.where((k // 2) ^ p[2] == n, k % 2, 0), 2 * p[1] + m)

        return pl.BlockSpec((HD2, mrow), im)

    pspec = pl.BlockSpec((HD2, ROWS), lambda m, k, p: (k, 0))
    outs = [CHIP, ROWS, ROWS]
    return pl.pallas_call(
        gqkv_kernel,
        grid_spec=pltpu.PrefetchScalarGridSpec(
            num_scalar_prefetch=1,
            grid=(2, 8),
            in_specs=[hspec(n) for n in range(POOL)] + [pspec] * POOL,
            out_specs=[pl.BlockSpec((mrow, w), lambda m, k, p: (m, 0)) for w in outs],
            scratch_shapes=[pltpu.VMEM((mrow, SEQ), F32)],
        ),
        out_shape=[jax.ShapeDtypeStruct((half, w), BF) for w in outs],
        compiler_params=params(2),
        cost_estimate=cost(2 * seq * half * SEQ, seq * SEQ * POOL + half * SEQ * 2),
        name="grad_wqkv",
    )(sc, *hids, *parts)


def dhid_kernel(sc, p0, p1, s0, s1, wq, wk, wv, xa, xb, dya, dyb, bs, gain, dm_ref, dx_ref, gp_ref, dq_s, dk_s, dv_s, dh_s):
    i = pl.program_id(0)
    nb = pl.num_programs(0) // 2
    own_chip = (i // nb) == sc[0]
    c = sc[1]
    for t, part in enumerate((p0, p1, s0, s1)):
        cc = c if t < 2 else 1 - c
        g = t % 2
        dq_s[:, pl.ds(pl.multiple_of(cc * ROWS + HD2 * g, HD2), HD2)] = part[:, :HD2]
        kv = pl.ds(pl.multiple_of(cc * HD2 + HD * g, HD), HD)
        dk_s[:, kv] = part[:, HD2:768]
        dv_s[:, kv] = part[:, 768:]
    for n in range(5):
        sl = slice(HD2 * n, HD2 * n + HD2)
        acc = dot_nt(dq_s[ALL], wq[sl, :])
        acc = acc + dot_nt(dk_s[ALL], wk[sl, :])
        acc = acc + dot_nt(dv_s[ALL], wv[sl, :])
        dh_s[:, sl] = acc.astype(BF).astype(F32)
    dh = dh_s[ALL]
    x = jnp.where(own_chip, xa[ALL], xb[ALL]).astype(F32)
    rs = lax.rsqrt(jnp.mean(x * x, axis=1, keepdims=YES) + EPS)
    n = x * rs
    g1 = ONE + gain[ALL]
    dhn = dh * n

    @pl.when(i == 0)
    def _():
        gp_ref[ALL] = jnp.zeros_like(gp_ref)

    gp_ref[ALL] += jnp.sum(dhn, axis=0, keepdims=YES)
    mean = jnp.mean(dhn * g1, axis=1, keepdims=YES)
    dx = ((dh * g1 - n * mean) * rs).astype(BF).astype(F32)
    dy = jnp.where(own_chip, dya[ALL], dyb[ALL]).astype(F32)
    dm = (dy + dx).astype(BF)
    dm_ref[ALL] = dm

    @pl.when(own_chip)
    def _():
        dx_ref[ALL] = jnp.where(bs[ALL] >= 0, jnp.zeros_like(dm), dm)


def dhid_call(sc, parts, wq, wk, wv, x_mine, x_peer, dy_mine, dy_peer, bs_col, gain):
    rows, d = x_mine.shape
    rb = HD
    nb = rows // rb

    def prow(i, s):
        return ((i // nb) * 2 + s[1]) * nb + i % nb

    def own(i, s):
        return (jnp.clip(i - nb * s[0], 0, nb - 1), 0)

    def peer(i, s):
        return (jnp.clip(i - nb * (1 - s[0]), 0, nb - 1), 0)

    pspec = pl.BlockSpec((rb, ROWS), lambda i, s: (prow(i, s), 0))
    return pl.pallas_call(
        dhid_kernel,
        grid_spec=pltpu.PrefetchScalarGridSpec(
            num_scalar_prefetch=1,
            grid=(2 * nb,),
            in_specs=[pspec] * POOL
            + [const_spec(wq.shape), const_spec(wk.shape), const_spec(wv.shape)]
            + [pl.BlockSpec((rb, d), own), pl.BlockSpec((rb, d), peer)] * 2
            + [pl.BlockSpec((rb, 1), lambda i, s: (prow(i, s), 0)), const_spec((1, d))],
            out_specs=[
                pl.BlockSpec((rb, d), lambda i, s: (i, 0)),
                pl.BlockSpec((rb, d), own),
                pl.BlockSpec((1, d), lambda i, s: (0, 0)),
            ],
            scratch_shapes=[
                pltpu.VMEM((rb, CHIP), BF),
                pltpu.VMEM((rb, ROWS), BF),
                pltpu.VMEM((rb, ROWS), BF),
                pltpu.VMEM((rb, d), F32),
            ],
        ),
        out_shape=[
            jax.ShapeDtypeStruct((2 * rows, d), BF),
            jax.ShapeDtypeStruct((rows, d), BF),
            jax.ShapeDtypeStruct((1, d), F32),
        ],
        compiler_params=params(1),
        cost_estimate=cost(2 * 2 * rows * d * SEQ, rows * 2 * d * 8 + d * SEQ * 2),
        name="d_hidden",
    )(sc, *parts, wq, wk, wv, x_mine, x_peer, dy_mine, dy_peer, bs_col, gain)


def dsoft_kernel(sc, own_ref, sib_ref, out_ref, buf, sem):
    n = pl.program_id(0)
    c = sc[0]
    last = pl.num_programs(0) - 1

    def copies(im, slot, act):
        for t in range(2):
            b = jnp.minimum(sc[1 + im] + t, 15)
            r = b // POOL
            row = pl.multiple_of(((r // 2) * POOL + b % POOL) * HD, HD)
            dst = buf.at[slot, pl.ds(HD * t, HD), :]
            mine = (r % 2) == c

            @pl.when(mine)
            def _():
                cp = pltpu.make_async_copy(own_ref.at[pl.ds(row, HD), :], dst, sem.at[slot, t])
                cp.start() if act == "start" else cp.wait()

            @pl.when(jnp.logical_not(mine))
            def _():
                cp = pltpu.make_async_copy(sib_ref.at[pl.ds(row, HD), :], dst, sem.at[slot, t])
                cp.start() if act == "start" else cp.wait()

    @pl.when(n == 0)
    def _():
        copies(0, 0, "start")

    @pl.when(n < last)
    def _():
        copies(n + 1, (n + 1) % 2, "start")

    slot = n % 2
    copies(n, slot, "wait")
    off = sc[9 + n]
    row = lax.broadcasted_iota(jnp.int32, (HD, HD2), 0)
    col = lax.broadcasted_iota(jnp.int32, (HD, HD2), 1)
    pick = jnp.where(col == row + off, ONE, 0.0).astype(BF)
    out_ref[ALL] = dot(pick, buf[slot]).astype(BF)


def dsoft_call(sc, dm_own, dm_sib):
    d = dm_own.shape[1]
    return pl.pallas_call(
        dsoft_kernel,
        grid_spec=pltpu.PrefetchScalarGridSpec(
            num_scalar_prefetch=1,
            grid=(8,),
            in_specs=[ANY, ANY],
            out_specs=pl.BlockSpec((HD, d), lambda n, s: (n, 0)),
            scratch_shapes=[pltpu.VMEM((2, HD2, d), BF), pltpu.SemaphoreType.DMA((2, 2))],
        ),
        out_shape=jax.ShapeDtypeStruct((CHIP, d), BF),
        compiler_params=params(1),
        cost_estimate=cost(2 * CHIP * HD2 * d, 3 * CHIP * d * 2),
        name="d_soft",
    )(sc, dm_own, dm_sib)


def dvis_kernel(sc, ds_ref, wp, pooled_ref, gain, out_ref, gp_ref, dp_s):
    i = pl.program_id(0)

    @pl.when(i == 0)
    def _():
        dn = dot_nt(ds_ref[ALL], wp[ALL]).astype(BF).astype(F32)
        pv = pooled_ref[ALL].astype(F32)
        rs = lax.rsqrt(jnp.mean(pv * pv, axis=1, keepdims=YES) + EPS)
        n = pv * rs
        g1 = ONE + gain[ALL]
        dnn = dn * n
        gp_ref[ALL] = jnp.sum(dnn, axis=0, keepdims=YES)
        mean = jnp.mean(dnn * g1, axis=1, keepdims=YES)
        dp_s[ALL] = (((dn * g1 - n * mean) * rs).astype(BF).astype(F32) * (ONE / 16.0)).astype(BF)

    row = lax.broadcasted_iota(jnp.int32, (ROWS, GRID), 0)
    tok = lax.broadcasted_iota(jnp.int32, (ROWS, GRID), 1)
    hit = (tok // SIDE == row // HD) & (tok % SIDE == (row % GRID) // POOL)
    mask = jnp.where(hit, ONE, 0.0).astype(BF)
    out_ref[0] = dot(mask, dp_s[pl.ds(pl.multiple_of(i * GRID, GRID), GRID), :]).astype(BF)


def dvis_call(sc, d_soft, wp, pooled, gain):
    n, dv = pooled.shape
    d = d_soft.shape[1]
    return pl.pallas_call(
        dvis_kernel,
        grid_spec=pltpu.PrefetchScalarGridSpec(
            num_scalar_prefetch=1,
            grid=(n // GRID,),
            in_specs=[
                pl.BlockSpec((n, d), lambda i, s: (s[0], 0), pipeline_mode=pl.Buffered(1)),
                const_spec(wp.shape),
                const_spec(pooled.shape),
                const_spec((1, dv)),
            ],
            out_specs=[pl.BlockSpec((1, ROWS, dv), lambda i, s: (i // POOL, i % POOL, 0)), pl.BlockSpec((1, dv), lambda i, s: (0, 0))],
            scratch_shapes=[pltpu.VMEM((n, dv), BF)],
        ),
        out_shape=[jax.ShapeDtypeStruct((n // BLK, GRID * GRID, dv), BF), jax.ShapeDtypeStruct((1, dv), F32)],
        compiler_params=params(1),
        cost_estimate=cost(2 * n * d * dv + 2 * n * SIDE * HD * dv, n * SIDE * dv * 2 + wp.size * 2),
        name="d_vis",
    )(sc, d_soft, wp, pooled, gain)


def solution(mesh):
    seq_spec = P(('dp', 'cp'))
    part_spec = P('dp')
    rep_spec = P()

    def body(vis, text, img_pos, grad_y, pn_gain, w_proj, pre_gain, w_query, w_key, w_value, q_gain, k_gain, w_out, post_gain):
        rank = lax.axis_index('cp')
        x = rank // 2
        c = rank % 2
        seq = POOL * text.shape[0]
        row_f32 = lambda g: g.astype(F32)[jnp.newaxis, :]
        xswap = lambda a: lax.ppermute(a, 'cp', XPERM)
        sswap = lambda a: lax.ppermute(a, 'cp', SPERM)
        ints = lambda *v: jnp.stack([jnp.asarray(e, jnp.int32) for e in v])

        pos = img_pos.astype(jnp.int32)
        ids = jnp.arange(8, dtype=jnp.int32)
        start = (jnp.arange(SIDE, dtype=jnp.int32) * HD)[:, jnp.newaxis]
        at_a = (pos[jnp.newaxis] <= start) & (pos[jnp.newaxis] + BLK > start)
        at_b = (pos[jnp.newaxis] > start) & (pos[jnp.newaxis] < start + HD)

        def pick(hit):
            idx = jnp.sum(jnp.where(hit, ids[jnp.newaxis], 0), axis=1)
            shift = jnp.where(jnp.any(hit, axis=1), start[:, 0] - jnp.sum(jnp.where(hit, pos[jnp.newaxis], 0), axis=1), FAR)
            return idx, shift

        ia, da = pick(at_a)
        ib, db = pick(at_b)
        tab = jnp.stack([ia, da, ib, db], axis=1).reshape(-1)
        rows = jnp.arange(seq, dtype=jnp.int32)
        inside = (rows[:, jnp.newaxis] >= pos[jnp.newaxis]) & (rows[:, jnp.newaxis] < pos[jnp.newaxis] + BLK)
        blk_start = jnp.where(jnp.any(inside, axis=1), jnp.sum(jnp.where(inside, pos[jnp.newaxis], 0), axis=1), -FAR)
        bs_col = blk_start[:, jnp.newaxis]
        bs_row = blk_start.reshape(seq // QB, 1, QB)
        qb_lo = jnp.arange(seq // QB, dtype=jnp.int32) * QB
        cross = (pos[jnp.newaxis] < (qb_lo + QB)[:, jnp.newaxis]) & (pos[jnp.newaxis] + BLK > (qb_lo + QB)[:, jnp.newaxis])
        cross = jnp.any(cross, axis=1).astype(jnp.int32)
        nblk = jnp.arange(seq // QB, dtype=jnp.int32)
        nkv = nblk + 1 + cross
        first_q = nblk - jnp.concatenate([jnp.zeros((1,), jnp.int32), cross[:-1]])

        inv_freq = ROPE_BASE ** (-jnp.arange(0, HD, 2).astype(F32) / HD)
        angle = (rows.astype(F32) / ROPE_SCALE)[:, jnp.newaxis] * inv_freq[jnp.newaxis, :]
        cos, sin = jnp.cos(angle), jnp.sin(angle)

        pooled, normed = pool_call(vis, row_f32(pn_gain))
        normed_x = xswap(normed)
        text_in, _ = lax.optimization_barrier((text, normed))
        text_x = xswap(text_in)
        mine = jnp.stack([normed, normed_x])
        theirs = sswap(mine)
        normed_all = jnp.zeros((POOL,) + normed.shape, BF)
        normed_all = lax.dynamic_update_index_in_dim(normed_all, normed, rank, 0)
        normed_all = lax.dynamic_update_index_in_dim(normed_all, normed_x, rank ^ 2, 0)
        normed_all = lax.dynamic_update_index_in_dim(normed_all, theirs[0], rank ^ 1, 0)
        normed_all = lax.dynamic_update_index_in_dim(normed_all, theirs[1], rank ^ 3, 0)
        normed_all = normed_all.reshape(-1, normed.shape[1])
        soft = jnp.dot(normed_all, w_proj, preferred_element_type=F32).astype(BF)

        pre = row_f32(pre_gain)
        qg, kg = row_f32(q_gain), row_f32(k_gain)
        x_mine, h_mine = merge_call(tab, ints(rank), soft, text, pre)
        h_sib = sswap(h_mine)
        qkv_args = (w_query, w_key, w_value, qg, kg, cos, sin)
        bufs = qkv_call(ints(x, c), h_mine, h_sib, *qkv_args, None)
        x_peer, h_peer = merge_call(tab, ints(rank ^ 2), soft, text_x, pre)
        h_diag = sswap(h_peer)
        dy_in, _ = lax.optimization_barrier((grad_y, text_x))
        dy_x = xswap(dy_in)
        q0, q1, qr0, qr1, k0, k1, kr0, kr1, v0, v1 = qkv_call(ints(1 - x, c), h_peer, h_diag, *qkv_args, bufs)

        o0, lse0 = fwd_call(nkv, q0, k0, v0, bs_col)
        o0s = sswap(o0)
        o1, lse1 = fwd_call(nkv, q1, k1, v1, bs_col)
        o1s = sswap(o1)

        post = row_f32(post_gain)
        y, dp_m, dam0, dam1, das0, das1, gpost_m = out_call(ints(x, c), (o0, o1), (o0s, o1s), w_out, x_mine, grad_y, post, YES)
        dp_p, dap0, dap1, dbs0, dbs1, gpost_p = out_call(ints(1 - x, c), (o0, o1), (o0s, o1s), w_out, x_peer, dy_x, post, False)

        def pair(m, p):
            return jnp.stack([jnp.where(x == 0, m, p), jnp.where(x == 0, p, m)])

        do0, do1 = pair(dam0, dap0), pair(dam1, dap1)
        do0s, do1s = sswap(pair(das0, dbs0)), sswap(pair(das1, dbs1))
        bsc = jnp.concatenate([ints(c), first_q])
        bwd_args = (cos, sin, qg, kg)
        part0, gq0, gk0 = bwd_call(bsc, q0, do0, do0s, o0, k0, v0, lse0, bs_row, qr0, kr0, *bwd_args)
        part0s = sswap(part0)
        part1, gq1, gk1 = bwd_call(bsc, q1, do1, do1s, o1, k1, v1, lse1, bs_row, qr1, kr1, *bwd_args)
        part1s = sswap(part1)

        dp_sm, dp_sp = sswap(dp_m), sswap(dp_p)
        first = lambda m, p: jnp.where(x == 0, m, p)
        dps = (first(dp_m, dp_p), first(dp_p, dp_m), first(dp_sm, dp_sp), first(dp_sp, dp_sm))
        g_out = gwo_call(ints(x, c), o0, o1, dps)
        g_out = lax.all_gather(g_out, 'cp', axis_index_groups=[[0, 2, 1, 3]], tiled=YES)

        parts = (part0, part1, part0s, part1s)
        gq, gk, gv = gqkv_call(ints(x, c, rank), (h_mine, h_sib, h_peer, h_diag), parts)
        sib_gather = lambda a: lax.all_gather(a, 'cp', axis_index_groups=[[0, 1], [2, 3]], tiled=YES)
        gq, gk, gv = sib_gather(gq), sib_gather(gk), sib_gather(gv)

        dm, grad_text, gpre = dhid_call(ints(x, c), parts, w_query, w_key, w_value, x_mine, x_peer, grad_y, dy_x, bs_col, pre)
        dm_s = sswap(dm)
        d_soft = dsoft_call(jnp.concatenate([ints(c), pos // HD, pos % HD]), dm, dm_s)
        grad_vis, gpn = dvis_call(ints(rank), d_soft, w_proj, pooled, row_f32(pn_gain))
        g_proj = lax.dot_general(normed_all, d_soft, (((0,), (0,)), ((), ())), preferred_element_type=F32).astype(BF)

        once = lambda a: jnp.where(x == 0, a, 0.0)
        small = [gpn, once(gpre), once(gq0 + gq1), once(gk0 + gk1), once(gpost_m + gpost_p)]
        sizes = [a.shape[1] for a in small]
        summed = lax.psum(jnp.concatenate(small, axis=1)[0], 'cp').astype(BF)
        cuts = [sum(sizes[:n]) for n in range(6)]
        spn, spre, sq, sk, spost = [summed[cuts[n] : cuts[n + 1]] for n in range(5)]
        return (y, grad_text, grad_vis, spn, g_proj, spre, gq, gk, gv, sq, sk, g_out, spost)

    in_specs = (seq_spec, seq_spec, part_spec, seq_spec) + (rep_spec,) * 10
    out_specs = (seq_spec, seq_spec, seq_spec) + (part_spec,) * 10
    return jax.shard_map(body, mesh=mesh, in_specs=in_specs, out_specs=out_specs, check_vma=False)
```

```python
import functools
import jax
import jax.numpy as jnp
from jax import lax
from jax.experimental import pallas as pl
from jax.experimental.pallas import tpu as pltpu
from jax.sharding import PartitionSpec as P


GRID = 64
POOL = 4
SIDE = GRID // POOL
BLK = SIDE * SIDE
HD = 256
HD2 = 2 * HD
HD3 = 3 * HD
NBUF = 10
ROWS = 1024
CHIP = 2 * ROWS
SEQ = 2 * CHIP
LANES = 128
YES = True
ALL = ...
ONE = 1.0
EPS = 1e-6
ROPE_BASE = 1000000.0
ROPE_SCALE = 8.0
NEG_BIG = -1e30
LOG2E = 1.4426950408889634
BF = jnp.bfloat16
F32 = jnp.float32
FAR = 1 << 20
SLOT = (0, 2, 1, 3)
VMEM_MAX = 67043328

XPERM = [(0, 2), (2, 0), (1, 3), (3, 1)]
SPERM = [(0, 1), (1, 0), (2, 3), (3, 2)]


def dot(a, b):
    return lax.dot_general(a, b, (((1,), (0,)), ((), ())), preferred_element_type=F32)


def dot_nt(a, b):
    return lax.dot_general(a, b, (((1,), (1,)), ((), ())), preferred_element_type=F32)


def dot_tn(a, b):
    return lax.dot_general(a, b, (((0,), (0,)), ((), ())), preferred_element_type=F32)


def params(n_grid, **kw):
    return pltpu.CompilerParams(dimension_semantics=("arbitrary",) * n_grid, vmem_limit_bytes=kw.pop("vmem", VMEM_MAX - (1 << 20)), **kw)


def cost(flops, nbytes):
    return pl.CostEstimate(flops=int(flops), bytes_accessed=int(nbytes), transcendentals=0)


def const_spec(shape):
    return pl.BlockSpec(shape, lambda *a: (0,) * len(shape), pipeline_mode=pl.Buffered(1))


ANY = pl.BlockSpec(memory_space=pl.ANY)


def const_out(shape):
    return pl.BlockSpec(shape, lambda *a: (0,) * len(shape))


def pool_kernel(vis_ref, gain_ref, pooled_ref, normed_ref):
    row = lax.broadcasted_iota(jnp.int32, (GRID, ROWS), 0)
    src = lax.broadcasted_iota(jnp.int32, (GRID, ROWS), 1)
    hit = (row // SIDE == src // HD) & (row % SIDE == (src % GRID) // POOL)
    mask = jnp.where(hit, ONE, 0.0).astype(BF)
    pooled = (dot(mask, vis_ref[0]) * (ONE / 16.0)).astype(BF)
    pooled_ref[ALL] = pooled
    wide = pooled.astype(F32)
    rs = lax.rsqrt(jnp.mean(wide * wide, axis=1, keepdims=YES) + EPS)
    normed_ref[ALL] = (wide * rs * (ONE + gain_ref[ALL])).astype(BF)


def pool_call(vis, gain):
    n, _, dv = vis.shape
    return pl.pallas_call(
        pool_kernel,
        grid=(n * POOL,),
        in_specs=[pl.BlockSpec((1, ROWS, dv), lambda i: (i // POOL, i % POOL, 0)), const_spec((1, dv))],
        out_specs=[pl.BlockSpec((GRID, dv), lambda i: (i, 0))] * 2,
        out_shape=[jax.ShapeDtypeStruct((n * BLK, dv), BF)] * 2,
        compiler_params=params(1),
        cost_estimate=cost(2 * HD2 * ROWS * dv, vis.size * 2),
        name="pool",
    )(vis, gain)


def merge_kernel(tab, sc, soft, text, gain, x_ref, h_ref):
    b = sc[0] * POOL + pl.program_id(0)
    ia, da, ib, db = tab[POOL * b], tab[POOL * b + 1], tab[POOL * b + 2], tab[POOL * b + 3]
    some = (da < FAR) | (db < FAR)

    @pl.when(some)
    def _():
        row = lax.broadcasted_iota(jnp.int32, (HD, HD), 0)
        col = lax.broadcasted_iota(jnp.int32, (HD, HD), 1)
        pa = jnp.where(col == row + da, ONE, 0.0).astype(BF)
        pb = jnp.where(col == row + db, ONE, 0.0).astype(BF)
        sa = soft[pl.ds(pl.multiple_of(ia * HD, HD), HD), :]
        sb = soft[pl.ds(pl.multiple_of(ib * HD, HD), HD), :]
        val = (dot(pa, sa) + dot(pb, sb)).astype(BF)
        r1 = lax.broadcasted_iota(jnp.int32, (HD, 1), 0)
        ina = (r1 + da >= 0) & (r1 + da < HD)
        inb = (r1 + db >= 0) & (r1 + db < HD)
        x_ref[ALL] = jnp.where(ina | inb, val, text[ALL])

    @pl.when(jnp.logical_not(some))
    def _():
        x_ref[ALL] = text[ALL]

    xv = x_ref[ALL].astype(F32)
    rs = lax.rsqrt(jnp.mean(xv * xv, axis=1, keepdims=YES) + EPS)
    h_ref[ALL] = (xv * rs * (ONE + gain[ALL])).astype(BF)


def merge_call(tab, rr, soft, text, gain):
    rows, d = text.shape
    spec = pl.BlockSpec((HD, d), lambda i, *_: (i, 0))
    return pl.pallas_call(
        merge_kernel,
        grid_spec=pltpu.PrefetchScalarGridSpec(
            num_scalar_prefetch=2,
            grid=(rows // HD,),
            in_specs=[const_spec(soft.shape), spec, const_spec((1, d))],
            out_specs=[spec, spec],
        ),
        out_shape=[jax.ShapeDtypeStruct((rows, d), BF)] * 2,
        compiler_params=params(1),
        cost_estimate=cost(2 * rows * HD2 * d, (rows * 3 + soft.shape[0]) * d * 2),
        name="merge",
    )(tab, rr, soft, text, gain)


def rope_fwd(raw, gain, cos, sin):
    rs = lax.rsqrt(jnp.mean(raw * raw, axis=1, keepdims=YES) + EPS)
    n = raw * rs * (ONE + gain)
    a, b = n[:, :LANES], n[:, LANES:]
    return jnp.concatenate([a * cos - b * sin, b * cos + a * sin], axis=1)


def qkv_kernel(sc, ha, hb, wq, wk, wv, qg, kg, cos_ref, sin_ref, *rest):
    outs = rest[-NBUF:]
    q_o, qr_o, k_o, kr_o, v_o = outs[0:2], outs[2:POOL], outs[POOL:6], outs[6:8], outs[8:NBUF]
    hid = jnp.where(pl.program_id(0) < 2, ha[ALL], hb[ALL])
    cos, sin = cos_ref[ALL], sin_ref[ALL]
    for g in range(2):
        aq = dot(hid, wq[:, HD2 * g : HD2 * g + HD2]).astype(BF)
        qr_o[g][ALL] = aq
        for h in range(2):
            raw = aq[:, HD * h : HD * h + HD].astype(F32)
            q_o[g][:, HD * h : HD * h + HD] = (rope_fwd(raw, qg[ALL], cos, sin) * 0.0625).astype(BF)
        ak = dot(hid, wk[:, HD * g : HD * g + HD]).astype(BF)
        kr_o[g][ALL] = ak
        k_o[g][ALL] = rope_fwd(ak.astype(F32), kg[ALL], cos, sin).astype(BF)
        v_o[g][ALL] = dot(hid, wv[:, HD * g : HD * g + HD]).astype(BF)


def qkv_call(sc, ha, hb, wq, wk, wv, qg, kg, cos, sin, bufs):
    d = ha.shape[1]
    rows = HD2

    def outrow(i, s):
        return s[0] * POOL + jnp.where(i < 2, s[1] * 2 + i, (1 - s[1]) * 2 + i - 2)

    def ospec(w):
        return pl.BlockSpec((rows, w), lambda i, s: (outrow(i, s), 0))

    one = dict(pipeline_mode=pl.Buffered(1))
    widths = [HD2, HD2, HD2, HD2, HD, HD, HD, HD, HD, HD]
    in_specs = [
        pl.BlockSpec((rows, d), lambda i, s: (jnp.minimum(i, 1), 0)),
        pl.BlockSpec((rows, d), lambda i, s: (jnp.maximum(i - 2, 0), 0)),
        pl.BlockSpec((d, ROWS), lambda i, s: (0, s[1]), **one),
        pl.BlockSpec((d, HD2), lambda i, s: (0, s[1]), **one),
        pl.BlockSpec((d, HD2), lambda i, s: (0, s[1]), **one),
        const_spec((1, HD)),
        const_spec((1, HD)),
        ospec(LANES),
        ospec(LANES),
    ]
    args = [sc, ha, hb, wq, wk, wv, qg, kg, cos, sin]
    alias = {}
    if bufs:
        alias = {len(args) + n: n for n in range(NBUF)}
        in_specs += [ANY] * NBUF
        args += list(bufs)
    seq = POOL * ha.shape[0]
    return pl.pallas_call(
        qkv_kernel,
        grid_spec=pltpu.PrefetchScalarGridSpec(
            num_scalar_prefetch=1, grid=(POOL,), in_specs=in_specs, out_specs=[ospec(w) for w in widths]
        ),
        out_shape=[jax.ShapeDtypeStruct((seq, w), BF) for w in widths],
        input_output_aliases=alias,
        compiler_params=params(1),
        cost_estimate=cost(2 * CHIP * d * CHIP, CHIP * (d + 3584) * 2 + d * CHIP * 2),
        name="qkv",
    )(*args)


QB = 512
KB = 512


def fwd_kernel(nkv, q_ref, k_ref, v_ref, bs_ref, o_ref, lse_ref, m_s, l_s, acc_s):
    i = pl.program_id(0)
    m_s[ALL] = jnp.full(m_s.shape, NEG_BIG, F32)
    l_s[ALL] = jnp.zeros(l_s.shape, F32)
    acc_s[ALL] = jnp.zeros(acc_s.shape, F32)

    def step(j, masked):
        off = pl.multiple_of(j * KB, KB)
        kb = k_ref[pl.ds(off, KB), :]
        vb = v_ref[pl.ds(off, KB), :]
        if masked:
            qpos = i * QB + lax.broadcasted_iota(jnp.int32, (QB, KB), 0)
            kpos = j * KB + lax.broadcasted_iota(jnp.int32, (QB, KB), 1)
            rel = kpos - bs_ref[ALL]
            vis = (kpos <= qpos) | ((rel >= 0) & (rel < BLK))
        ss = [dot_nt(q_ref[:, HD * h : HD * h + HD], kb) for h in range(2)]
        for h in range(2):
            s = ss[h]
            if masked:
                s = jnp.where(vis, s, NEG_BIG)
            parts = [s[:, LANES * t : LANES * t + LANES] for t in range(KB // LANES)]
            mx = functools.reduce(jnp.maximum, parts)
            mx = jnp.broadcast_to(jnp.max(mx, axis=1, keepdims=YES), (QB, LANES))
            m_old = m_s[h]
            m_new = jnp.maximum(m_old, mx)
            alpha = jnp.exp2((m_old - m_new) * LOG2E)
            ps = [jnp.exp2((t - m_new) * LOG2E) for t in parts]
            l_s[h] = l_s[h] * alpha + functools.reduce(jnp.add, ps)
            m_s[h] = m_new
            p = jnp.concatenate([t.astype(BF) for t in ps], axis=1)
            acc_s[h] = acc_s[h] * jnp.concatenate([alpha, alpha], axis=1) + dot(p, vb)

    lax.fori_loop(0, i, lambda j, c: (step(j, False), c)[1], 0)
    step(i, YES)

    @pl.when(nkv[i] > i + 1)
    def _():
        step(i + 1, YES)

    for h in range(2):
        l = jnp.broadcast_to(jnp.sum(l_s[h], axis=1, keepdims=YES), (QB, LANES))
        inv = ONE / l
        o_ref[:, HD * h : HD * h + HD] = (acc_s[h] * jnp.concatenate([inv, inv], axis=1)).astype(BF)
        lse = m_s[h] * LOG2E + jnp.log2(l)
        lse_ref[0, h : h + 1, :] = jnp.transpose(lse)[0:1, :]


def fwd_call(nkv, q, k, v, bs_col):
    seq = q.shape[0]
    n = seq // QB
    return pl.pallas_call(
        fwd_kernel,
        grid_spec=pltpu.PrefetchScalarGridSpec(
            num_scalar_prefetch=1,
            grid=(n,),
            in_specs=[
                pl.BlockSpec((QB, HD2), lambda i, *_: (i, 0)),
                const_spec((seq, HD)),
                const_spec((seq, HD)),
                pl.BlockSpec((QB, 1), lambda i, *_: (i, 0)),
            ],
            out_specs=[pl.BlockSpec((QB, HD2), lambda i, *_: (i, 0)), pl.BlockSpec((1, 2, QB), lambda i, *_: (i, 0, 0))],
            scratch_shapes=[pltpu.VMEM((2, QB, LANES), F32), pltpu.VMEM((2, QB, LANES), F32), pltpu.VMEM((2, QB, HD), F32)],
        ),
        out_shape=[jax.ShapeDtypeStruct((seq, HD2), BF), jax.ShapeDtypeStruct((n, 2, QB), F32)],
        compiler_params=params(1),
        cost_estimate=cost(2 * 2 * 2 * seq * seq * HD * 0.7, seq * 1536 * 2),
        name="attn_fwd",
    )(nkv, q, k, v, bs_col)


def out_kernel(sc, oo0, oo1, os0, os1, wo, dy_ref, gain, *rest):
    x_ref, y_ref = rest[:2] if len(rest) == 8 else (None, None)
    dp_ref, da_o0, da_o1, da_s0, da_s1, gp_ref = rest[-6:]
    c = sc[1]
    own = pl.multiple_of(c * ROWS, ROWS)
    sib = pl.multiple_of((1 - c) * ROWS, ROWS)
    a = dot(oo0[ALL], wo[pl.ds(own, HD2), :])
    a = a + dot(oo1[ALL], wo[pl.ds(own + HD2, HD2), :])
    a = a + dot(os0[ALL], wo[pl.ds(sib, HD2), :])
    a = a + dot(os1[ALL], wo[pl.ds(sib + HD2, HD2), :])
    a = a.astype(BF).astype(F32)
    rs = lax.rsqrt(jnp.mean(a * a, axis=1, keepdims=YES) + EPS)
    g1 = ONE + gain[ALL]
    n = a * rs
    if y_ref is not None:
        y_ref[ALL] = (x_ref[ALL].astype(F32) + n * g1).astype(BF)
    dy = dy_ref[ALL].astype(F32)
    dyn = dy * n

    @pl.when(pl.program_id(0) == 0)
    def _():
        gp_ref[ALL] = jnp.zeros_like(gp_ref)

    gp_ref[ALL] += jnp.sum(dyn, axis=0, keepdims=YES)
    mean = jnp.mean(dyn * g1, axis=1, keepdims=YES)
    dp = ((dy * g1 - n * mean) * rs).astype(BF)
    dp_ref[ALL] = dp
    da_o0[ALL] = dot_nt(dp, wo[pl.ds(own, HD2), :]).astype(BF)
    da_o1[ALL] = dot_nt(dp, wo[pl.ds(own + HD2, HD2), :]).astype(BF)
    da_s0[ALL] = dot_nt(dp, wo[pl.ds(sib, HD2), :]).astype(BF)
    da_s1[ALL] = dot_nt(dp, wo[pl.ds(sib + HD2, HD2), :]).astype(BF)


def out_call(sc, oo, osib, wo, dy, gain, x=()):
    rows, d = dy.shape
    rb = HD
    nb = rows // rb

    def orow(i, s):
        return (s[0] * 2 + s[1]) * nb + i

    ospec = pl.BlockSpec((rb, HD2), lambda i, s: (orow(i, s), 0))
    rspec = pl.BlockSpec((rb, d), lambda i, s: (i, 0))
    pspec = pl.BlockSpec((rb, HD2), lambda i, s: (i, 0))
    extra = len(x)
    return pl.pallas_call(
        out_kernel,
        grid_spec=pltpu.PrefetchScalarGridSpec(
            num_scalar_prefetch=1,
            grid=(nb,),
            in_specs=[ospec] * POOL + [const_spec(wo.shape), rspec, const_spec((1, d))] + [rspec] * extra,
            out_specs=[rspec] * (1 + extra) + [pspec] * POOL + [const_out((1, d))],
        ),
        out_shape=[jax.ShapeDtypeStruct((rows, d), BF)] * (1 + extra)
        + [jax.ShapeDtypeStruct((rows, HD2), BF)] * POOL
        + [jax.ShapeDtypeStruct((1, d), F32)],
        compiler_params=params(1),
        cost_estimate=cost(POOL * rows * d * CHIP, rows * d * 2 * 5 + wo.size * 2),
        name="out_proj",
    )(sc, oo[0], oo[1], osib[0], osib[1], wo, dy, gain, *x)


def rope_norm_bwd(dy, raw, gain, cos, sin):
    d1, d2 = dy[:, :LANES], dy[:, LANES:]
    dn = jnp.concatenate([d1 * cos + d2 * sin, d2 * cos - d1 * sin], axis=1)
    rs = lax.rsqrt(jnp.mean(raw * raw, axis=1, keepdims=YES) + EPS)
    n = raw * rs
    dnn = dn * n
    gg = jnp.sum(dnn, axis=0, keepdims=YES)
    mean = jnp.mean(dnn * (ONE + gain), axis=1, keepdims=YES)
    return ((dn * (ONE + gain) - n * mean) * rs).astype(BF), gg


def bwd_kernel(
    sc, q_ref, do_a, do_b, do_c, do_d, o_ref, k_ref, v_ref, lse_ref, bs_ref, qr_ref, kr_ref, cos_ref, sin_ref, qg, kg,
    out_ref, gq_ref, gk_ref, do_s, dl_s, dq_s, dk_s, dv_s, sem,
):
    j = pl.program_id(0)
    nj = pl.num_programs(0)

    @pl.when(j == 0)
    def _():
        cps = []
        for n, src in enumerate((do_a, do_b, do_c, do_d)):
            row = pl.multiple_of((sc[0] ^ SLOT[n]) * ROWS, ROWS)
            cps.append(pltpu.make_async_copy(src, do_s.at[pl.ds(row, ROWS), :], sem.at[n]))
        for cp in cps:
            cp.start()
        dq_s[ALL] = jnp.zeros_like(dq_s)
        gq_ref[ALL] = jnp.zeros_like(gq_ref)
        gk_ref[ALL] = jnp.zeros_like(gk_ref)
        for cp in cps:
            cp.wait()

        def delta(i, carry):
            off = pl.multiple_of(i * QB, QB)
            pr = do_s[pl.ds(off, QB), :].astype(F32) * o_ref[pl.ds(off, QB), :].astype(F32)
            for h in range(2):
                col = jnp.sum(pr[:, HD * h : HD * h + HD], axis=1, keepdims=YES)
                dl_s[i, h : h + 1, :] = jnp.transpose(jnp.broadcast_to(col, (QB, LANES)))[0:1, :]
            return carry

        lax.fori_loop(0, SEQ // QB, delta, 0)

    dk_s[ALL] = jnp.zeros_like(dk_s)
    dv_s[ALL] = jnp.zeros_like(dv_s)
    kb = k_ref[ALL]
    vb = v_ref[ALL]

    def step(i, masked):
        off = pl.multiple_of(i * QB, QB)
        if masked:
            kpos = j * KB + lax.broadcasted_iota(jnp.int32, (KB, QB), 0)
            qpos = i * QB + lax.broadcasted_iota(jnp.int32, (KB, QB), 1)
            rel = kpos - bs_ref[i]
            vis = (kpos <= qpos) | ((rel >= 0) & (rel < BLK))
        qs = [q_ref[pl.ds(off, QB), HD * h : HD * h + HD] for h in range(2)]
        dos = [do_s[pl.ds(off, QB), HD * h : HD * h + HD] for h in range(2)]
        st = [dot_nt(kb, qs[h]) for h in range(2)]
        dpt = [dot_nt(vb, dos[h]) for h in range(2)]
        for h in range(2):
            pt = jnp.exp2(st[h] * LOG2E - lse_ref[i, h : h + 1, :])
            if masked:
                pt = jnp.where(vis, pt, 0.0)
            dst = (pt * (dpt[h] - dl_s[i, h : h + 1, :])).astype(BF)
            dv_s[ALL] += dot(pt.astype(BF), dos[h])
            dk_s[ALL] += dot(dst, qs[h])
            dq_s[pl.ds(off, QB), HD * h : HD * h + HD] += dot_tn(dst, kb)

    @pl.when(sc[1 + j] < j)
    def _():
        step(jnp.maximum(j - 1, 0), YES)

    step(j, YES)
    lax.fori_loop(j + 1, nj, lambda i, cr: (step(i, False), cr)[1], 0)

    koff = pl.multiple_of(j * KB, KB)
    dk, gk = rope_norm_bwd(
        dk_s[ALL].astype(BF).astype(F32), kr_ref[ALL].astype(F32), kg[ALL], cos_ref[pl.ds(koff, KB), :], sin_ref[pl.ds(koff, KB), :]
    )
    gk_ref[ALL] += gk
    out_ref[pl.ds(koff, KB), HD2:HD3] = dk
    out_ref[pl.ds(koff, KB), HD3:ROWS] = dv_s[ALL].astype(BF)

    @pl.when(j == nj - 1)
    def _():
        def fin(i, carry):
            off = pl.multiple_of(i * HD, HD)
            cos, sin = cos_ref[pl.ds(off, HD), :], sin_ref[pl.ds(off, HD), :]
            for h in range(2):
                sl = slice(HD * h, HD * h + HD)
                dq = (dq_s[pl.ds(off, HD), sl] * 0.0625).astype(BF).astype(F32)
                dqr, gq = rope_norm_bwd(dq, qr_ref[pl.ds(off, HD), sl].astype(F32), qg[ALL], cos, sin)
                gq_ref[ALL] += gq
                out_ref[pl.ds(off, HD), sl] = dqr
            return carry

        lax.fori_loop(0, SEQ // HD, fin, 0)


def bwd_call(sc, q, dos, o, k, v, lse, bs_row, qr, kr, cos, sin, qg, kg):
    seq = q.shape[0]
    nj = seq // KB
    return pl.pallas_call(
        bwd_kernel,
        grid_spec=pltpu.PrefetchScalarGridSpec(
            num_scalar_prefetch=1,
            grid=(nj,),
            in_specs=[
                const_spec((seq, HD2)),
                ANY,
                ANY,
                ANY,
                ANY,
                const_spec((seq, HD2)),
                pl.BlockSpec((KB, HD), lambda j, *_: (j, 0)),
                pl.BlockSpec((KB, HD), lambda j, *_: (j, 0)),
                const_spec(lse.shape),
                const_spec(bs_row.shape),
                const_spec((seq, HD2)),
                pl.BlockSpec((KB, HD), lambda j, *_: (j, 0)),
                const_spec((seq, LANES)),
                const_spec((seq, LANES)),
                const_spec((1, HD)),
                const_spec((1, HD)),
            ],
            out_specs=[
                pl.BlockSpec((seq, ROWS), lambda j, *_: (0, 0)),
                pl.BlockSpec((1, HD), lambda j, *_: (0, 0)),
                pl.BlockSpec((1, HD), lambda j, *_: (0, 0)),
            ],
            scratch_shapes=[
                pltpu.VMEM((seq, HD2), BF),
                pltpu.VMEM((seq // QB, 2, QB), F32),
                pltpu.VMEM((seq, HD2), F32),
                pltpu.VMEM((KB, HD), F32),
                pltpu.VMEM((KB, HD), F32),
                pltpu.SemaphoreType.DMA((POOL,)),
            ],
        ),
        out_shape=[
            jax.ShapeDtypeStruct((seq, ROWS), BF),
            jax.ShapeDtypeStruct((1, HD), F32),
            jax.ShapeDtypeStruct((1, HD), F32),
        ],
        compiler_params=params(1),
        cost_estimate=cost(5 * 2 * 2 * seq * seq * HD * 0.6, seq * 4000 * 2),
        name="attn_bwd",
    )(sc, q, *dos, o, k, v, lse, bs_row, qr, kr, cos, sin, qg, kg)


def gwo_kernel(sc, o0, o1, dp0, dp1, dp2, dp3, out_ref, full_ref, acc):
    s = pl.program_id(0)
    o = jnp.where(sc[0] == 0, o0[ALL], o1[ALL])

    @pl.when(s == 0)
    def _():
        acc[ALL] = jnp.zeros_like(acc)

    for n, ref in enumerate((dp0, dp1, dp2, dp3)):

        @pl.when(s // 2 == n)
        def _():
            acc[ALL] += dot_tn(o, ref[ALL])

    @pl.when(s == pl.num_programs(0) - 1)
    def _():
        out_ref[ALL] = acc[ALL].astype(BF)
        full_ref[ALL] = acc[ALL].astype(BF)


def gwo_call(sc, o0, o1, dps):
    seq = o0.shape[0]
    d = dps[0].shape[1]
    ospec = pl.BlockSpec((HD2, HD2), lambda s, p: (p[3 + s // 2] * 2 + s % 2, 0))
    dspecs = [pl.BlockSpec((HD2, d), lambda s, p, n=n: (jnp.clip(s - 2 * n, 0, 1), 0)) for n in range(POOL)]
    return pl.pallas_call(
        gwo_kernel,
        grid_spec=pltpu.PrefetchScalarGridSpec(
            num_scalar_prefetch=1,
            grid=(8,),
            in_specs=[ospec, ospec] + dspecs,
            out_specs=[const_out((HD2, d)), pl.BlockSpec((HD2, d), lambda s, p: (2 * p[1] + p[0], 0))],
            scratch_shapes=[pltpu.VMEM((HD2, d), F32)],
        ),
        out_shape=[jax.ShapeDtypeStruct((HD2, d), BF), jax.ShapeDtypeStruct((CHIP, d), BF)],
        compiler_params=params(1),
        cost_estimate=cost(2 * seq * HD2 * d, seq * (d + ROWS) * 2),
        name="grad_wo",
    )(sc, o0, o1, *dps)


def gqkv_kernel(sc, h0, h1, h2, h3, p0, p1, s0, s1, gq_ref, gk_ref, gv_ref, fq_ref, fk_ref, fv_ref, acc):
    k = pl.program_id(1)
    c = sc[1]

    @pl.when(k == 0)
    def _():
        acc[ALL] = jnp.zeros_like(acc)

    r = k // 2
    xr = r ^ sc[2]
    for n, ref in enumerate((h0, h1, h2, h3)):

        @pl.when(xr == n)
        def _():
            h = ref[ALL]
            for t, part in enumerate((p0, p1, s0, s1)):
                acc[:, ROWS * t : ROWS * t + ROWS] += dot_tn(h, part[ALL])

    @pl.when(k == pl.num_programs(1) - 1)
    def _():
        for t in range(POOL):
            cc = c if t < 2 else 1 - c
            g = t % 2
            base = ROWS * t
            qc = pl.ds(pl.multiple_of(cc * ROWS + HD2 * g, HD2), HD2)
            kv = pl.ds(pl.multiple_of(cc * HD2 + HD * g, HD), HD)
            vq = acc[:, base : base + HD2].astype(BF)
            vk = acc[:, base + HD2 : base + HD2 + HD].astype(BF)
            vv = acc[:, base + HD2 + HD : base + ROWS].astype(BF)
            for ref, cols, val in ((gq_ref, qc, vq), (fq_ref, qc, vq), (gk_ref, kv, vk), (fk_ref, kv, vk), (gv_ref, kv, vv), (fv_ref, kv, vv)):
                ref[:, cols] = val


def gqkv_call(sc, hids, parts):
    seq = parts[0].shape[0]
    half = hids[0].shape[1] // 2
    mrow = half // 2

    def hspec(n):
        def im(m, k, p):
            return (jnp.where((k // 2) ^ p[2] == n, k % 2, 0), 2 * p[1] + m)

        return pl.BlockSpec((HD2, mrow), im)

    pspec = pl.BlockSpec((HD2, ROWS), lambda m, k, p: (k, 0))
    outs = [CHIP, ROWS, ROWS]
    return pl.pallas_call(
        gqkv_kernel,
        grid_spec=pltpu.PrefetchScalarGridSpec(
            num_scalar_prefetch=1,
            grid=(2, 8),
            in_specs=[hspec(n) for n in range(POOL)] + [pspec] * POOL,
            out_specs=[pl.BlockSpec((mrow, w), lambda m, k, p: (m, 0)) for w in outs]
            + [pl.BlockSpec((mrow, w), lambda m, k, p: (2 * p[1] + m, 0)) for w in outs],
            scratch_shapes=[pltpu.VMEM((mrow, SEQ), F32)],
        ),
        out_shape=[jax.ShapeDtypeStruct((half, w), BF) for w in outs] + [jax.ShapeDtypeStruct((2 * half, w), BF) for w in outs],
        compiler_params=params(2),
        cost_estimate=cost(2 * seq * half * SEQ, seq * SEQ * POOL + half * SEQ * 2),
        name="grad_wqkv",
    )(sc, *hids, *parts)


def dhid_kernel(sc, p0, p1, s0, s1, wq, wk, wv, xa, xb, dya, dyb, bs, gain, dm_ref, dx_ref, gp_ref, dq_s, dk_s, dv_s, dh_s):
    i = pl.program_id(0)
    nb = pl.num_programs(0) // 2
    own_chip = (i // nb) == sc[0]
    c = sc[1]
    for t, part in enumerate((p0, p1, s0, s1)):
        cc = c if t < 2 else 1 - c
        g = t % 2
        dq_s[:, pl.ds(pl.multiple_of(cc * ROWS + HD2 * g, HD2), HD2)] = part[:, :HD2]
        kv = pl.ds(pl.multiple_of(cc * HD2 + HD * g, HD), HD)
        dk_s[:, kv] = part[:, HD2:HD3]
        dv_s[:, kv] = part[:, HD3:]
    for n in range(5):
        sl = slice(HD2 * n, HD2 * n + HD2)
        acc = dot_nt(dq_s[ALL], wq[sl, :])
        acc = acc + dot_nt(dk_s[ALL], wk[sl, :])
        acc = acc + dot_nt(dv_s[ALL], wv[sl, :])
        dh_s[:, sl] = acc.astype(BF).astype(F32)
    dh = dh_s[ALL]
    x = jnp.where(own_chip, xa[ALL], xb[ALL]).astype(F32)
    rs = lax.rsqrt(jnp.mean(x * x, axis=1, keepdims=YES) + EPS)
    n = x * rs
    g1 = ONE + gain[ALL]
    dhn = dh * n

    @pl.when(i == 0)
    def _():
        gp_ref[ALL] = jnp.zeros_like(gp_ref)

    gp_ref[ALL] += jnp.sum(dhn, axis=0, keepdims=YES)
    mean = jnp.mean(dhn * g1, axis=1, keepdims=YES)
    dx = ((dh * g1 - n * mean) * rs).astype(BF).astype(F32)
    dy = jnp.where(own_chip, dya[ALL], dyb[ALL]).astype(F32)
    dm = (dy + dx).astype(BF)
    dm_ref[ALL] = dm

    @pl.when(own_chip)
    def _():
        dx_ref[ALL] = jnp.where(bs[ALL] >= 0, jnp.zeros_like(dm), dm)


def dhid_call(sc, parts, wq, wk, wv, x_mine, x_peer, dy_mine, dy_peer, bs_col, gain):
    rows, d = x_mine.shape
    rb = HD
    nb = rows // rb

    def prow(i, s):
        return ((i // nb) * 2 + s[1]) * nb + i % nb

    def own(i, s):
        return (jnp.clip(i - nb * s[0], 0, nb - 1), 0)

    def peer(i, s):
        return (jnp.clip(i - nb * (1 - s[0]), 0, nb - 1), 0)

    pspec = pl.BlockSpec((rb, ROWS), lambda i, s: (prow(i, s), 0))
    return pl.pallas_call(
        dhid_kernel,
        grid_spec=pltpu.PrefetchScalarGridSpec(
            num_scalar_prefetch=1,
            grid=(2 * nb,),
            in_specs=[pspec] * POOL
            + [const_spec(wq.shape), const_spec(wk.shape), const_spec(wv.shape)]
            + [pl.BlockSpec((rb, d), own), pl.BlockSpec((rb, d), peer)] * 2
            + [pl.BlockSpec((rb, 1), lambda i, s: (prow(i, s), 0)), const_spec((1, d))],
            out_specs=[
                pl.BlockSpec((rb, d), lambda i, s: (i, 0)),
                pl.BlockSpec((rb, d), own),
                pl.BlockSpec((1, d), lambda i, s: (0, 0)),
            ],
            scratch_shapes=[
                pltpu.VMEM((rb, CHIP), BF),
                pltpu.VMEM((rb, ROWS), BF),
                pltpu.VMEM((rb, ROWS), BF),
                pltpu.VMEM((rb, d), F32),
            ],
        ),
        out_shape=[
            jax.ShapeDtypeStruct((2 * rows, d), BF),
            jax.ShapeDtypeStruct((rows, d), BF),
            jax.ShapeDtypeStruct((1, d), F32),
        ],
        compiler_params=params(1),
        cost_estimate=cost(2 * 2 * rows * d * SEQ, rows * 2 * d * 8 + d * SEQ * 2),
        name="d_hidden",
    )(sc, *parts, wq, wk, wv, x_mine, x_peer, dy_mine, dy_peer, bs_col, gain)


def dsoft_kernel(sc, own_ref, sib_ref, out_ref, buf, sem):
    n = pl.program_id(0)
    c = sc[0]
    last = pl.num_programs(0) - 1

    def copies(im, slot, act):
        for t in range(2):
            b = jnp.minimum(sc[1 + im] + t, 15)
            r = b // POOL
            row = pl.multiple_of(((r // 2) * POOL + b % POOL) * HD, HD)
            dst = buf.at[slot, pl.ds(HD * t, HD), :]
            mine = (r % 2) == c

            @pl.when(mine)
            def _():
                cp = pltpu.make_async_copy(own_ref.at[pl.ds(row, HD), :], dst, sem.at[slot, t])
                cp.start() if act == "start" else cp.wait()

            @pl.when(jnp.logical_not(mine))
            def _():
                cp = pltpu.make_async_copy(sib_ref.at[pl.ds(row, HD), :], dst, sem.at[slot, t])
                cp.start() if act == "start" else cp.wait()

    @pl.when(n == 0)
    def _():
        copies(0, 0, "start")

    @pl.when(n < last)
    def _():
        copies(n + 1, (n + 1) % 2, "start")

    slot = n % 2
    copies(n, slot, "wait")
    off = sc[9 + n]
    row = lax.broadcasted_iota(jnp.int32, (HD, HD2), 0)
    col = lax.broadcasted_iota(jnp.int32, (HD, HD2), 1)
    pick = jnp.where(col == row + off, ONE, 0.0).astype(BF)
    out_ref[ALL] = dot(pick, buf[slot]).astype(BF)


def dsoft_call(sc, dm_own, dm_sib):
    d = dm_own.shape[1]
    return pl.pallas_call(
        dsoft_kernel,
        grid_spec=pltpu.PrefetchScalarGridSpec(
            num_scalar_prefetch=1,
            grid=(8,),
            in_specs=[ANY, ANY],
            out_specs=pl.BlockSpec((HD, d), lambda n, s: (n, 0)),
            scratch_shapes=[pltpu.VMEM((2, HD2, d), BF), pltpu.SemaphoreType.DMA((2, 2))],
        ),
        out_shape=jax.ShapeDtypeStruct((CHIP, d), BF),
        compiler_params=params(1),
        cost_estimate=cost(2 * CHIP * HD2 * d, 3 * CHIP * d * 2),
        name="d_soft",
    )(sc, dm_own, dm_sib)


def dvis_kernel(sc, ds_ref, wp, pooled_ref, gain, out_ref, gp_ref, dp_s):
    i = pl.program_id(0)

    @pl.when(i == 0)
    def _():
        dn = dot_nt(ds_ref[ALL], wp[ALL]).astype(BF).astype(F32)
        pv = pooled_ref[ALL].astype(F32)
        rs = lax.rsqrt(jnp.mean(pv * pv, axis=1, keepdims=YES) + EPS)
        n = pv * rs
        g1 = ONE + gain[ALL]
        dnn = dn * n
        gp_ref[ALL] = jnp.sum(dnn, axis=0, keepdims=YES)
        mean = jnp.mean(dnn * g1, axis=1, keepdims=YES)
        dp_s[ALL] = (((dn * g1 - n * mean) * rs).astype(BF).astype(F32) * (ONE / 16.0)).astype(BF)

    row = lax.broadcasted_iota(jnp.int32, (ROWS, GRID), 0)
    tok = lax.broadcasted_iota(jnp.int32, (ROWS, GRID), 1)
    hit = (tok // SIDE == row // HD) & (tok % SIDE == (row % GRID) // POOL)
    mask = jnp.where(hit, ONE, 0.0).astype(BF)
    out_ref[0] = dot(mask, dp_s[pl.ds(pl.multiple_of(i * GRID, GRID), GRID), :]).astype(BF)


def dvis_call(sc, d_soft, wp, pooled, gain):
    n, dv = pooled.shape
    d = d_soft.shape[1]
    return pl.pallas_call(
        dvis_kernel,
        grid_spec=pltpu.PrefetchScalarGridSpec(
            num_scalar_prefetch=1,
            grid=(n // GRID,),
            in_specs=[
                pl.BlockSpec((n, d), lambda i, s: (s[0], 0), pipeline_mode=pl.Buffered(1)),
                const_spec(wp.shape),
                const_spec(pooled.shape),
                const_spec((1, dv)),
            ],
            out_specs=[pl.BlockSpec((1, ROWS, dv), lambda i, s: (i // POOL, i % POOL, 0)), pl.BlockSpec((1, dv), lambda i, s: (0, 0))],
            scratch_shapes=[pltpu.VMEM((n, dv), BF)],
        ),
        out_shape=[jax.ShapeDtypeStruct((n // BLK, GRID * GRID, dv), BF), jax.ShapeDtypeStruct((1, dv), F32)],
        compiler_params=params(1),
        cost_estimate=cost(2 * n * d * dv + 2 * n * SIDE * HD * dv, n * SIDE * dv * 2 + wp.size * 2),
        name="d_vis",
    )(sc, d_soft, wp, pooled, gain)


def tail_kernel(sc, normed, ds, sq, sk, sv, go_x, go_s, go_d, fq_in, fk_in, fv_in, fo_in, out_ref, fq, fk, fv, fo, sem):
    i = pl.program_id(0)
    row = pl.multiple_of(sc[0] + i * HD, HD)
    orow = jnp.minimum(i, 3) * LANES
    cps = [pltpu.make_async_copy(src, dst.at[pl.ds(row, HD), :], sem.at[n]) for n, (src, dst) in enumerate(((sq, fq), (sk, fk), (sv, fv)))]
    for n, src in enumerate((go_x, go_s, go_d)):
        at = pl.multiple_of(sc[1 + n] + orow, LANES)
        cps.append(pltpu.make_async_copy(src, fo.at[pl.ds(at, LANES), :], sem.at[3 + n]))
    for cp in cps:
        cp.start()
    out_ref[ALL] = dot_tn(normed[ALL], ds[ALL]).astype(BF)
    for cp in cps:
        cp.wait()


def tail_call(sc, normed, ds, halves, quarters, fulls):
    tok, dv = normed.shape
    d = ds.shape[1]
    half = lambda w: pl.BlockSpec((HD, w), lambda i, s: (i, 0))
    quarter = pl.BlockSpec((LANES, d), lambda i, s: (jnp.minimum(i, 3), 0))
    return pl.pallas_call(
        tail_kernel,
        grid_spec=pltpu.PrefetchScalarGridSpec(
            num_scalar_prefetch=1,
            grid=(5,),
            in_specs=[const_spec(normed.shape), pl.BlockSpec((tok, HD2), lambda i, s: (0, i))]
            + [half(h.shape[1]) for h in halves]
            + [quarter] * 3
            + [ANY] * POOL,
            out_specs=[pl.BlockSpec((dv, HD2), lambda i, s: (0, i))] + [ANY] * POOL,
            scratch_shapes=[pltpu.SemaphoreType.DMA((6,))],
        ),
        out_shape=[jax.ShapeDtypeStruct((dv, d), BF)] + [jax.ShapeDtypeStruct(f.shape, BF) for f in fulls],
        input_output_aliases={9 + n: 1 + n for n in range(POOL)},
        compiler_params=params(1),
        cost_estimate=cost(2 * tok * dv * d, tok * (d + dv) * 2 + dv * d * 2),
        name="tail",
    )(sc, normed, ds, *halves, *quarters, *fulls)


def solution(mesh):
    seq_spec = P(('dp', 'cp'))
    part_spec = P('dp')
    rep_spec = P()

    def body(vis, text, img_pos, grad_y, pn_gain, w_proj, pre_gain, w_query, w_key, w_value, q_gain, k_gain, w_out, post_gain):
        rank = lax.axis_index('cp')
        x = rank // 2
        c = rank % 2
        seq = POOL * text.shape[0]
        row_f32 = lambda g: g.astype(F32)[jnp.newaxis, :]
        ints = lambda *v: jnp.stack([jnp.asarray(e, jnp.int32) for e in v])

        pos = img_pos.astype(jnp.int32)
        ids = jnp.arange(8, dtype=jnp.int32)
        start = (jnp.arange(SIDE, dtype=jnp.int32) * HD)[:, jnp.newaxis]
        at_a = (pos[jnp.newaxis] <= start) & (pos[jnp.newaxis] + BLK > start)
        at_b = (pos[jnp.newaxis] > start) & (pos[jnp.newaxis] < start + HD)

        def pick(hit):
            idx = jnp.sum(jnp.where(hit, ids[jnp.newaxis], 0), axis=1)
            shift = jnp.where(jnp.any(hit, axis=1), start[:, 0] - jnp.sum(jnp.where(hit, pos[jnp.newaxis], 0), axis=1), FAR)
            return idx, shift

        ia, da = pick(at_a)
        ib, db = pick(at_b)
        tab = jnp.stack([ia, da, ib, db], axis=1).reshape(-1)
        rows = jnp.arange(seq, dtype=jnp.int32)
        inside = (rows[:, jnp.newaxis] >= pos[jnp.newaxis]) & (rows[:, jnp.newaxis] < pos[jnp.newaxis] + BLK)
        blk_start = jnp.where(jnp.any(inside, axis=1), jnp.sum(jnp.where(inside, pos[jnp.newaxis], 0), axis=1), -FAR)
        bs_col = blk_start[:, jnp.newaxis]
        bs_row = blk_start.reshape(seq // QB, 1, QB)
        qb_lo = jnp.arange(seq // QB, dtype=jnp.int32) * QB
        cross = (pos[jnp.newaxis] < (qb_lo + QB)[:, jnp.newaxis]) & (pos[jnp.newaxis] + BLK > (qb_lo + QB)[:, jnp.newaxis])
        cross = jnp.any(cross, axis=1).astype(jnp.int32)
        nblk = jnp.arange(seq // QB, dtype=jnp.int32)
        nkv = nblk + 1 + cross
        first_q = nblk - jnp.concatenate([jnp.zeros((1,), jnp.int32), cross[:-1]])

        def swap(a, perm):
            return lax.ppermute(a, 'cp', perm)

        pooled, normed = pool_call(vis, row_f32(pn_gain))
        normed_x = swap(normed, XPERM)
        text_x = swap(text, XPERM)
        dy_x = swap(grad_y, XPERM)
        theirs = swap(jnp.stack([normed, normed_x]), SPERM)
        normed_all = jnp.zeros((POOL,) + normed.shape, BF)
        for piece, slot in ((normed, 0), (normed_x, 2), (theirs[0], 1), (theirs[1], 3)):
            normed_all = lax.dynamic_update_index_in_dim(normed_all, piece, rank ^ slot, 0)
        normed_all = normed_all.reshape(-1, normed.shape[1])
        soft = jnp.dot(normed_all, w_proj, preferred_element_type=F32).astype(BF)

        pre = row_f32(pre_gain)
        qg, kg = row_f32(q_gain), row_f32(k_gain)
        x_mine, h_mine = merge_call(tab, ints(rank), soft, text, pre)
        h_sib = swap(h_mine, SPERM)
        inv_freq = ROPE_BASE ** (-jnp.arange(0, HD, 2).astype(F32) / HD)
        angle = (rows.astype(F32) / ROPE_SCALE)[:, jnp.newaxis] * inv_freq[jnp.newaxis, :]
        cos, sin = jnp.cos(angle), jnp.sin(angle)
        qkv_args = (w_query, w_key, w_value, qg, kg, cos, sin)
        bufs = qkv_call(ints(x, c), h_mine, h_sib, *qkv_args, ())
        x_peer, h_peer = merge_call(tab, ints(rank ^ 2), soft, text_x, pre)
        h_diag = swap(h_peer, SPERM)
        q0, q1, qr0, qr1, k0, k1, kr0, kr1, v0, v1 = qkv_call(ints(1 - x, c), h_peer, h_diag, *qkv_args, bufs)

        o0, lse0 = fwd_call(nkv, q0, k0, v0, bs_col)
        o0s = swap(o0, SPERM)
        o1, lse1 = fwd_call(nkv, q1, k1, v1, bs_col)
        o1s = swap(o1, SPERM)

        post = row_f32(post_gain)
        y, dp_m, dam0, dam1, das0, das1, gpost_m = out_call(ints(x, c), (o0, o1), (o0s, o1s), w_out, grad_y, post, (x_mine,))
        das0, das1 = swap(das0, SPERM), swap(das1, SPERM)
        dp_sm = swap(dp_m, SPERM)
        dp_p, dap0, dap1, dbs0, dbs1, gpost_p = out_call(ints(1 - x, c), (o0, o1), (o0s, o1s), w_out, dy_x, post)
        dbs0, dbs1 = swap(dbs0, SPERM), swap(dbs1, SPERM)
        dp_sp = swap(dp_p, SPERM)

        bsc = jnp.concatenate([ints(rank), first_q])
        bwd_args = (cos, sin, qg, kg)
        part0, gq0, gk0 = bwd_call(bsc, q0, (dam0, dap0, das0, dbs0), o0, k0, v0, lse0, bs_row, qr0, kr0, *bwd_args)
        part0s = swap(part0, SPERM)
        part1, gq1, gk1 = bwd_call(bsc, q1, (dam1, dap1, das1, dbs1), o1, k1, v1, lse1, bs_row, qr1, kr1, *bwd_args)
        part1s = swap(part1, SPERM)

        go, go_full = gwo_call(ints(x, c, rank, *[rank ^ n for n in SLOT]), o0, o1, (dp_m, dp_p, dp_sm, dp_sp))
        go_x = swap(go, XPERM)
        go_s = swap(go, SPERM)
        early = jnp.concatenate([gq0 + gq1, gk0 + gk1, gpost_m + gpost_p], axis=1)
        early = early + swap(early, SPERM)

        parts = (part0, part1, part0s, part1s)
        dm, grad_text, gpre = dhid_call(ints(x, c), parts, w_query, w_key, w_value, x_mine, x_peer, grad_y, dy_x, bs_col, pre)
        dm_s = swap(dm, SPERM)
        gpre = gpre + swap(gpre, SPERM)
        go_d = swap(go_x, SPERM)
        *g_half, fq, fk, fv = gqkv_call(ints(x, c, rank), (h_mine, h_sib, h_peer, h_diag), parts)
        halves = [swap(a, SPERM) for a in g_half]
        d_soft = dsoft_call(jnp.concatenate([ints(c), pos // HD, pos % HD]), dm, dm_s)
        grad_vis, gpn = dvis_call(ints(rank), d_soft, w_proj, pooled, row_f32(pn_gain))
        gpn = gpn + swap(gpn, XPERM)
        gpn = gpn + swap(gpn, SPERM)
        where = ints((1 - c) * w_query.shape[0] // 2, (2 * c + 1 - x) * HD2, (2 - 2 * c + x) * HD2, (3 - 2 * c - x) * HD2)
        g_proj, gq, gk, gv, g_out = tail_call(where, normed_all, d_soft, halves, (go_x, go_s, go_d), (fq, fk, fv, go_full))

        early = early[0].astype(BF)
        sq, sk, spost = early[:HD], early[HD:HD2], early[HD2:]
        return (y, grad_text, grad_vis, gpn[0].astype(BF), g_proj, gpre[0].astype(BF), gq, gk, gv, sq, sk, g_out, spost)

    in_specs = (seq_spec, seq_spec, part_spec, seq_spec) + (rep_spec,) * NBUF
    out_specs = (seq_spec, seq_spec, seq_spec) + (part_spec,) * NBUF
    return jax.shard_map(body, mesh=mesh, in_specs=in_specs, out_specs=out_specs, check_vma=False)
```

```python
import functools
import jax
import jax.numpy as jnp
from jax import lax
from jax.experimental import pallas as pl
from jax.experimental.pallas import tpu as pltpu
from jax.sharding import PartitionSpec as P


GRID = 64
POOL = 4
SIDE = GRID // POOL
BLK = SIDE * SIDE
HD = 256
HD2 = 2 * HD
HD3 = 3 * HD
NBUF = 10
ROWS = 1024
CHIP = 2 * ROWS
SEQ = 2 * CHIP
LANES = 128
YES = True
ALL = ...
ONE = 1.0
EPS = 1e-6
ROPE_BASE = 1000000.0
ROPE_SCALE = 8.0
NEG_BIG = -1e30
LOG2E = 1.4426950408889634
BF = jnp.bfloat16
F32 = jnp.float32
MIB = 1 << 20
FAR = MIB
SLOT = (0, 2, 1, 3)
VMEM_MAX = 67043328

XPERM = [(0, 2), (2, 0), (1, 3), (3, 1)]
SPERM = [(0, 1), (1, 0), (2, 3), (3, 2)]


def pid():
    return pl.program_id(0)


def dot(a, b):
    return lax.dot_general(a, b, (((1,), (0,)), ((), ())), preferred_element_type=F32)


def dot_nt(a, b):
    return lax.dot_general(a, b, (((1,), (1,)), ((), ())), preferred_element_type=F32)


def dot_tn(a, b):
    return lax.dot_general(a, b, (((0,), (0,)), ((), ())), preferred_element_type=F32)


def params(n_grid, **kw):
    return pltpu.CompilerParams(dimension_semantics=("arbitrary",) * n_grid, vmem_limit_bytes=kw.pop("vmem", VMEM_MAX - MIB), **kw)


def cost(flops, nbytes):
    return pl.CostEstimate(flops=int(flops), bytes_accessed=int(nbytes), transcendentals=0)


def const_spec(shape):
    return pl.BlockSpec(shape, lambda *a: (0,) * len(shape), pipeline_mode=pl.Buffered(1))


ANY = pl.BlockSpec(memory_space=pl.ANY)


def const_out(shape):
    return pl.BlockSpec(shape, lambda *a: (0,) * len(shape))


def pool_kernel(vis_ref, gain_ref, pooled_ref, normed_ref):
    row = lax.broadcasted_iota(jnp.int32, (GRID, ROWS), 0)
    src = lax.broadcasted_iota(jnp.int32, (GRID, ROWS), 1)
    hit = (row // SIDE == src // HD) & (row % SIDE == (src % GRID) // POOL)
    mask = jnp.where(hit, ONE, 0.0).astype(BF)
    pooled = (dot(mask, vis_ref[0]) * (ONE / 16.0)).astype(BF)
    pooled_ref[ALL] = pooled
    wide = pooled.astype(F32)
    rs = lax.rsqrt(jnp.mean(wide * wide, axis=1, keepdims=YES) + EPS)
    normed_ref[ALL] = (wide * rs * (ONE + gain_ref[ALL])).astype(BF)


def pool_call(vis, gain):
    n, _, dv = vis.shape
    return pl.pallas_call(
        pool_kernel,
        grid=(n * POOL,),
        in_specs=[pl.BlockSpec((1, ROWS, dv), lambda i: (i // POOL, i % POOL, 0)), const_spec((1, dv))],
        out_specs=[pl.BlockSpec((GRID, dv), lambda i: (i, 0))] * 2,
        out_shape=[jax.ShapeDtypeStruct((n * BLK, dv), BF)] * 2,
        compiler_params=params(1, vmem=12 * MIB),
        cost_estimate=cost(2 * HD2 * ROWS * dv, vis.size * 2),
        name="pool",
    )(vis, gain)


def merge_kernel(tab, sc, soft, text, gain, x_ref, h_ref):
    b = sc[0] * POOL + pid()
    ia, da, ib, db = tab[POOL * b], tab[POOL * b + 1], tab[POOL * b + 2], tab[POOL * b + 3]
    some = (da < FAR) | (db < FAR)

    @pl.when(some)
    def _():
        row = lax.broadcasted_iota(jnp.int32, (HD, HD), 0)
        col = lax.broadcasted_iota(jnp.int32, (HD, HD), 1)
        pa = jnp.where(col == row + da, ONE, 0.0).astype(BF)
        pb = jnp.where(col == row + db, ONE, 0.0).astype(BF)
        sa = soft[pl.ds(pl.multiple_of(ia * HD, HD), HD), :]
        sb = soft[pl.ds(pl.multiple_of(ib * HD, HD), HD), :]
        val = (dot(pa, sa) + dot(pb, sb)).astype(BF)
        r1 = lax.broadcasted_iota(jnp.int32, (HD, 1), 0)
        ina = (r1 + da >= 0) & (r1 + da < HD)
        inb = (r1 + db >= 0) & (r1 + db < HD)
        x_ref[ALL] = jnp.where(ina | inb, val, text[ALL])

    @pl.when(jnp.logical_not(some))
    def _():
        x_ref[ALL] = text[ALL]

    xv = x_ref[ALL].astype(F32)
    rs = lax.rsqrt(jnp.mean(xv * xv, axis=1, keepdims=YES) + EPS)
    h_ref[ALL] = (xv * rs * (ONE + gain[ALL])).astype(BF)


def merge_call(tab, rr, soft, text, gain):
    rows, d = text.shape
    spec = pl.BlockSpec((HD, d), lambda i, *_: (i, 0))
    return pl.pallas_call(
        merge_kernel,
        grid_spec=pltpu.PrefetchScalarGridSpec(
            num_scalar_prefetch=2,
            grid=(rows // HD,),
            in_specs=[const_spec(soft.shape), spec, const_spec((1, d))],
            out_specs=[spec, spec],
        ),
        out_shape=[jax.ShapeDtypeStruct((rows, d), BF)] * 2,
        compiler_params=params(1, vmem=26 * MIB),
        cost_estimate=cost(2 * rows * HD2 * d, (rows * 3 + soft.shape[0]) * d * 2),
        name="merge",
    )(tab, rr, soft, text, gain)


def rope_fwd(raw, gain, cos, sin):
    rs = lax.rsqrt(jnp.mean(raw * raw, axis=1, keepdims=YES) + EPS)
    n = raw * rs * (ONE + gain)
    a, b = n[:, :LANES], n[:, LANES:]
    return jnp.concatenate([a * cos - b * sin, b * cos + a * sin], axis=1)


def qkv_kernel(sc, ha, hb, wq, wk, wv, qg, kg, cos_ref, sin_ref, *rest):
    outs = rest[-NBUF:]
    q_o, qr_o, k_o, kr_o, v_o = outs[0:2], outs[2:POOL], outs[POOL:6], outs[6:8], outs[8:NBUF]
    hid = jnp.where(pid() < 2, ha[ALL], hb[ALL])
    cos, sin = cos_ref[ALL], sin_ref[ALL]
    for g in range(2):
        aq = dot(hid, wq[:, HD2 * g : HD2 * g + HD2]).astype(BF)
        qr_o[g][ALL] = aq
        for h in range(2):
            raw = aq[:, HD * h : HD * h + HD].astype(F32)
            q_o[g][:, HD * h : HD * h + HD] = (rope_fwd(raw, qg[ALL], cos, sin) * 0.0625).astype(BF)
        ak = dot(hid, wk[:, HD * g : HD * g + HD]).astype(BF)
        kr_o[g][ALL] = ak
        k_o[g][ALL] = rope_fwd(ak.astype(F32), kg[ALL], cos, sin).astype(BF)
        v_o[g][ALL] = dot(hid, wv[:, HD * g : HD * g + HD]).astype(BF)


def qkv_call(sc, ha, hb, wq, wk, wv, qg, kg, cos, sin, bufs):
    d = ha.shape[1]
    rows = HD2

    def outrow(i, s):
        return s[0] * POOL + jnp.where(i < 2, s[1] * 2 + i, (1 - s[1]) * 2 + i - 2)

    def ospec(w):
        return pl.BlockSpec((rows, w), lambda i, s: (outrow(i, s), 0))

    one = dict(pipeline_mode=pl.Buffered(1))
    widths = [HD2, HD2, HD2, HD2, HD, HD, HD, HD, HD, HD]
    in_specs = [
        pl.BlockSpec((rows, d), lambda i, s: (jnp.minimum(i, 1), 0)),
        pl.BlockSpec((rows, d), lambda i, s: (jnp.maximum(i - 2, 0), 0)),
        pl.BlockSpec((d, ROWS), lambda i, s: (0, s[1]), **one),
        pl.BlockSpec((d, HD2), lambda i, s: (0, s[1]), **one),
        pl.BlockSpec((d, HD2), lambda i, s: (0, s[1]), **one),
        const_spec((1, HD)),
        const_spec((1, HD)),
        ospec(LANES),
        ospec(LANES),
    ]
    args = [sc, ha, hb, wq, wk, wv, qg, kg, cos, sin]
    alias = {}
    if bufs:
        alias = {len(args) + n: n for n in range(NBUF)}
        in_specs += [ANY] * NBUF
        args += list(bufs)
    seq = POOL * ha.shape[0]
    return pl.pallas_call(
        qkv_kernel,
        grid_spec=pltpu.PrefetchScalarGridSpec(
            num_scalar_prefetch=1, grid=(POOL,), in_specs=in_specs, out_specs=[ospec(w) for w in widths]
        ),
        out_shape=[jax.ShapeDtypeStruct((seq, w), BF) for w in widths],
        input_output_aliases=alias,
        compiler_params=params(1, vmem=40 * MIB),
        cost_estimate=cost(2 * CHIP * d * CHIP, CHIP * (d + 3584) * 2 + d * CHIP * 2),
        name="qkv",
    )(*args)


QB = 512
KB = 512


def fwd_kernel(nkv, q_ref, k_ref, v_ref, bs_ref, o_ref, lse_ref, m_s, l_s, acc_s):
    i = pid()
    m_s[ALL] = jnp.full(m_s.shape, NEG_BIG, F32)
    l_s[ALL] = jnp.zeros(l_s.shape, F32)
    acc_s[ALL] = jnp.zeros(acc_s.shape, F32)

    def step(j, masked):
        off = pl.multiple_of(j * KB, KB)
        kb = k_ref[pl.ds(off, KB), :]
        vb = v_ref[pl.ds(off, KB), :]
        if masked:
            qpos = i * QB + lax.broadcasted_iota(jnp.int32, (QB, KB), 0)
            kpos = j * KB + lax.broadcasted_iota(jnp.int32, (QB, KB), 1)
            rel = kpos - bs_ref[ALL]
            vis = (kpos <= qpos) | ((rel >= 0) & (rel < BLK))
        ss = [dot_nt(q_ref[:, HD * h : HD * h + HD], kb) for h in range(2)]
        for h in range(2):
            s = ss[h]
            if masked:
                s = jnp.where(vis, s, NEG_BIG)
            parts = [s[:, LANES * t : LANES * t + LANES] for t in range(KB // LANES)]
            mx = functools.reduce(jnp.maximum, parts)
            mx = jnp.broadcast_to(jnp.max(mx, axis=1, keepdims=YES), (QB, LANES))
            m_old = m_s[h]
            m_new = jnp.maximum(m_old, mx)
            alpha = jnp.exp2((m_old - m_new) * LOG2E)
            ps = [jnp.exp2((t - m_new) * LOG2E) for t in parts]
            l_s[h] = l_s[h] * alpha + functools.reduce(jnp.add, ps)
            m_s[h] = m_new
            p = jnp.concatenate([t.astype(BF) for t in ps], axis=1)
            acc_s[h] = acc_s[h] * jnp.concatenate([alpha, alpha], axis=1) + dot(p, vb)

    lax.fori_loop(0, i, lambda j, c: (step(j, False), c)[1], 0)
    step(i, YES)

    @pl.when(nkv[i] > i + 1)
    def _():
        step(i + 1, YES)

    for h in range(2):
        l = jnp.broadcast_to(jnp.sum(l_s[h], axis=1, keepdims=YES), (QB, LANES))
        inv = ONE / l
        o_ref[:, HD * h : HD * h + HD] = (acc_s[h] * jnp.concatenate([inv, inv], axis=1)).astype(BF)
        lse = m_s[h] * LOG2E + jnp.log2(l)
        lse_ref[0, h : h + 1, :] = jnp.transpose(lse)[0:1, :]


def fwd_call(nkv, q, k, v, bs_col):
    seq = q.shape[0]
    n = seq // QB
    return pl.pallas_call(
        fwd_kernel,
        grid_spec=pltpu.PrefetchScalarGridSpec(
            num_scalar_prefetch=1,
            grid=(n,),
            in_specs=[
                pl.BlockSpec((QB, HD2), lambda i, *_: (i, 0)),
                const_spec((seq, HD)),
                const_spec((seq, HD)),
                pl.BlockSpec((QB, 1), lambda i, *_: (i, 0)),
            ],
            out_specs=[pl.BlockSpec((QB, HD2), lambda i, *_: (i, 0)), pl.BlockSpec((1, 2, QB), lambda i, *_: (i, 0, 0))],
            scratch_shapes=[pltpu.VMEM((2, QB, LANES), F32), pltpu.VMEM((2, QB, LANES), F32), pltpu.VMEM((2, QB, HD), F32)],
        ),
        out_shape=[jax.ShapeDtypeStruct((seq, HD2), BF), jax.ShapeDtypeStruct((n, 2, QB), F32)],
        compiler_params=params(1, vmem=18 * MIB),
        cost_estimate=cost(2 * 2 * 2 * seq * seq * HD * 0.7, seq * 1536 * 2),
        name="attn_fwd",
    )(nkv, q, k, v, bs_col)


def out_kernel(sc, oo0, oo1, os0, os1, wo, dy_ref, gain, *rest):
    x_ref, y_ref = rest[:2] if len(rest) == 8 else (None, None)
    dp_ref, da_o0, da_o1, da_s0, da_s1, gp_ref = rest[-6:]
    c = sc[1]
    own = pl.multiple_of(c * ROWS, ROWS)
    sib = pl.multiple_of((1 - c) * ROWS, ROWS)
    a = dot(oo0[ALL], wo[pl.ds(own, HD2), :])
    a = a + dot(oo1[ALL], wo[pl.ds(own + HD2, HD2), :])
    a = a + dot(os0[ALL], wo[pl.ds(sib, HD2), :])
    a = a + dot(os1[ALL], wo[pl.ds(sib + HD2, HD2), :])
    a = a.astype(BF).astype(F32)
    rs = lax.rsqrt(jnp.mean(a * a, axis=1, keepdims=YES) + EPS)
    g1 = ONE + gain[ALL]
    n = a * rs
    if y_ref is not None:
        y_ref[ALL] = (x_ref[ALL].astype(F32) + n * g1).astype(BF)
    dy = dy_ref[ALL].astype(F32)
    dyn = dy * n

    @pl.when(pid() == 0)
    def _():
        gp_ref[ALL] = jnp.zeros_like(gp_ref)

    gp_ref[ALL] += jnp.sum(dyn, axis=0, keepdims=YES)
    mean = jnp.mean(dyn * g1, axis=1, keepdims=YES)
    dp = ((dy * g1 - n * mean) * rs).astype(BF)
    dp_ref[ALL] = dp
    da_o0[ALL] = dot_nt(dp, wo[pl.ds(own, HD2), :]).astype(BF)
    da_o1[ALL] = dot_nt(dp, wo[pl.ds(own + HD2, HD2), :]).astype(BF)
    da_s0[ALL] = dot_nt(dp, wo[pl.ds(sib, HD2), :]).astype(BF)
    da_s1[ALL] = dot_nt(dp, wo[pl.ds(sib + HD2, HD2), :]).astype(BF)


def out_call(sc, oo, osib, wo, dy, gain, x=()):
    rows, d = dy.shape
    rb = HD
    nb = rows // rb

    def orow(i, s):
        return (s[0] * 2 + s[1]) * nb + i

    ospec = pl.BlockSpec((rb, HD2), lambda i, s: (orow(i, s), 0))
    rspec = pl.BlockSpec((rb, d), lambda i, s: (i, 0))
    pspec = pl.BlockSpec((rb, HD2), lambda i, s: (i, 0))
    extra = len(x)
    return pl.pallas_call(
        out_kernel,
        grid_spec=pltpu.PrefetchScalarGridSpec(
            num_scalar_prefetch=1,
            grid=(nb,),
            in_specs=[ospec] * POOL + [const_spec(wo.shape), rspec, const_spec((1, d))] + [rspec] * extra,
            out_specs=[rspec] * (1 + extra) + [pspec] * POOL + [const_out((1, d))],
        ),
        out_shape=[jax.ShapeDtypeStruct((rows, d), BF)] * (1 + extra)
        + [jax.ShapeDtypeStruct((rows, HD2), BF)] * POOL
        + [jax.ShapeDtypeStruct((1, d), F32)],
        compiler_params=params(1, vmem=40 * MIB),
        cost_estimate=cost(POOL * rows * d * CHIP, rows * d * 2 * 5 + wo.size * 2),
        name="out_proj",
    )(sc, oo[0], oo[1], osib[0], osib[1], wo, dy, gain, *x)


def rope_norm_bwd(dy, raw, gain, cos, sin):
    d1, d2 = dy[:, :LANES], dy[:, LANES:]
    dn = jnp.concatenate([d1 * cos + d2 * sin, d2 * cos - d1 * sin], axis=1)
    rs = lax.rsqrt(jnp.mean(raw * raw, axis=1, keepdims=YES) + EPS)
    n = raw * rs
    dnn = dn * n
    gg = jnp.sum(dnn, axis=0, keepdims=YES)
    mean = jnp.mean(dnn * (ONE + gain), axis=1, keepdims=YES)
    return ((dn * (ONE + gain) - n * mean) * rs).astype(BF), gg


def bwd_kernel(
    sc, q_ref, do_a, do_b, do_c, do_d, o_ref, k_ref, v_ref, lse_ref, bs_ref, qr_ref, kr_ref, cos_ref, sin_ref, qg, kg,
    out_ref, gq_ref, gk_ref, do_s, dl_s, dq_s, dk_s, dv_s, sem,
):
    j = pid()
    nj = pl.num_programs(0)

    @pl.when(j == 0)
    def _():
        cps = []
        for n, src in enumerate((do_a, do_b, do_c, do_d)):
            row = pl.multiple_of((sc[0] ^ SLOT[n]) * ROWS, ROWS)
            cps.append(pltpu.make_async_copy(src, do_s.at[pl.ds(row, ROWS), :], sem.at[n]))
        for cp in cps:
            cp.start()
        dq_s[ALL] = jnp.zeros_like(dq_s)
        gq_ref[ALL] = jnp.zeros_like(gq_ref)
        gk_ref[ALL] = jnp.zeros_like(gk_ref)
        for cp in cps:
            cp.wait()

        def delta(i, carry):
            off = pl.multiple_of(i * QB, QB)
            pr = do_s[pl.ds(off, QB), :].astype(F32) * o_ref[pl.ds(off, QB), :].astype(F32)
            for h in range(2):
                col = jnp.sum(pr[:, HD * h : HD * h + HD], axis=1, keepdims=YES)
                dl_s[i, h : h + 1, :] = jnp.transpose(jnp.broadcast_to(col, (QB, LANES)))[0:1, :]
            return carry

        lax.fori_loop(0, SEQ // QB, delta, 0)

    dk_s[ALL] = jnp.zeros_like(dk_s)
    dv_s[ALL] = jnp.zeros_like(dv_s)
    kb = k_ref[ALL]
    vb = v_ref[ALL]

    def step(i, masked):
        off = pl.multiple_of(i * QB, QB)
        if masked:
            kpos = j * KB + lax.broadcasted_iota(jnp.int32, (KB, QB), 0)
            qpos = i * QB + lax.broadcasted_iota(jnp.int32, (KB, QB), 1)
            rel = kpos - bs_ref[i]
            vis = (kpos <= qpos) | ((rel >= 0) & (rel < BLK))
        qs = [q_ref[pl.ds(off, QB), HD * h : HD * h + HD] for h in range(2)]
        dos = [do_s[pl.ds(off, QB), HD * h : HD * h + HD] for h in range(2)]
        st = [dot_nt(kb, qs[h]) for h in range(2)]
        dpt = [dot_nt(vb, dos[h]) for h in range(2)]
        for h in range(2):
            pt = jnp.exp2(st[h] * LOG2E - lse_ref[i, h : h + 1, :])
            if masked:
                pt = jnp.where(vis, pt, 0.0)
            dst = (pt * (dpt[h] - dl_s[i, h : h + 1, :])).astype(BF)
            dv_s[ALL] += dot(pt.astype(BF), dos[h])
            dk_s[ALL] += dot(dst, qs[h])
            dq_s[pl.ds(off, QB), HD * h : HD * h + HD] += dot_tn(dst, kb)

    @pl.when(sc[1 + j] < j)
    def _():
        step(jnp.maximum(j - 1, 0), YES)

    step(j, YES)
    lax.fori_loop(j + 1, nj, lambda i, cr: (step(i, False), cr)[1], 0)

    koff = pl.multiple_of(j * KB, KB)
    dk, gk = rope_norm_bwd(
        dk_s[ALL].astype(BF).astype(F32), kr_ref[ALL].astype(F32), kg[ALL], cos_ref[pl.ds(koff, KB), :], sin_ref[pl.ds(koff, KB), :]
    )
    gk_ref[ALL] += gk
    out_ref[pl.ds(koff, KB), HD2:HD3] = dk
    out_ref[pl.ds(koff, KB), HD3:ROWS] = dv_s[ALL].astype(BF)

    @pl.when(j == nj - 1)
    def _():
        def fin(i, carry):
            off = pl.multiple_of(i * HD, HD)
            cos, sin = cos_ref[pl.ds(off, HD), :], sin_ref[pl.ds(off, HD), :]
            for h in range(2):
                sl = slice(HD * h, HD * h + HD)
                dq = (dq_s[pl.ds(off, HD), sl] * 0.0625).astype(BF).astype(F32)
                dqr, gq = rope_norm_bwd(dq, qr_ref[pl.ds(off, HD), sl].astype(F32), qg[ALL], cos, sin)
                gq_ref[ALL] += gq
                out_ref[pl.ds(off, HD), sl] = dqr
            return carry

        lax.fori_loop(0, SEQ // HD, fin, 0)


def bwd_call(sc, q, dos, o, k, v, lse, bs_row, qr, kr, cos, sin, qg, kg):
    seq = q.shape[0]
    nj = seq // KB
    return pl.pallas_call(
        bwd_kernel,
        grid_spec=pltpu.PrefetchScalarGridSpec(
            num_scalar_prefetch=1,
            grid=(nj,),
            in_specs=[
                const_spec((seq, HD2)),
                ANY,
                ANY,
                ANY,
                ANY,
                const_spec((seq, HD2)),
                pl.BlockSpec((KB, HD), lambda j, *_: (j, 0)),
                pl.BlockSpec((KB, HD), lambda j, *_: (j, 0)),
                const_spec(lse.shape),
                const_spec(bs_row.shape),
                const_spec((seq, HD2)),
                pl.BlockSpec((KB, HD), lambda j, *_: (j, 0)),
                const_spec((seq, LANES)),
                const_spec((seq, LANES)),
                const_spec((1, HD)),
                const_spec((1, HD)),
            ],
            out_specs=[
                pl.BlockSpec((seq, ROWS), lambda j, *_: (0, 0)),
                pl.BlockSpec((1, HD), lambda j, *_: (0, 0)),
                pl.BlockSpec((1, HD), lambda j, *_: (0, 0)),
            ],
            scratch_shapes=[
                pltpu.VMEM((seq, HD2), BF),
                pltpu.VMEM((seq // QB, 2, QB), F32),
                pltpu.VMEM((seq, HD2), F32),
                pltpu.VMEM((KB, HD), F32),
                pltpu.VMEM((KB, HD), F32),
                pltpu.SemaphoreType.DMA((POOL,)),
            ],
        ),
        out_shape=[
            jax.ShapeDtypeStruct((seq, ROWS), BF),
            jax.ShapeDtypeStruct((1, HD), F32),
            jax.ShapeDtypeStruct((1, HD), F32),
        ],
        compiler_params=params(1, vmem=53 * MIB),
        cost_estimate=cost(5 * 2 * 2 * seq * seq * HD * 0.6, seq * 4000 * 2),
        name="attn_bwd",
    )(sc, q, *dos, o, k, v, lse, bs_row, qr, kr, cos, sin, qg, kg)


def gwo_kernel(sc, o0, o1, dp0, dp1, dp2, dp3, out_ref, full_ref, acc):
    s = pid()
    o = jnp.where(sc[0] == 0, o0[ALL], o1[ALL])

    @pl.when(s == 0)
    def _():
        acc[ALL] = jnp.zeros_like(acc)

    for n, ref in enumerate((dp0, dp1, dp2, dp3)):

        @pl.when(s // 2 == n)
        def _():
            acc[ALL] += dot_tn(o, ref[ALL])

    @pl.when(s == pl.num_programs(0) - 1)
    def _():
        out_ref[ALL] = acc[ALL].astype(BF)
        full_ref[ALL] = acc[ALL].astype(BF)


def gwo_call(sc, o0, o1, dps):
    seq = o0.shape[0]
    d = dps[0].shape[1]
    ospec = pl.BlockSpec((HD2, HD2), lambda s, p: (p[3 + s // 2] * 2 + s % 2, 0))
    dspecs = [pl.BlockSpec((HD2, d), lambda s, p, n=n: (jnp.clip(s - 2 * n, 0, 1), 0)) for n in range(POOL)]
    return pl.pallas_call(
        gwo_kernel,
        grid_spec=pltpu.PrefetchScalarGridSpec(
            num_scalar_prefetch=1,
            grid=(8,),
            in_specs=[ospec, ospec] + dspecs,
            out_specs=[const_out((HD2, d)), pl.BlockSpec((HD2, d), lambda s, p: (2 * p[1] + p[0], 0))],
            scratch_shapes=[pltpu.VMEM((HD2, d), F32)],
        ),
        out_shape=[jax.ShapeDtypeStruct((HD2, d), BF), jax.ShapeDtypeStruct((CHIP, d), BF)],
        compiler_params=params(1, vmem=32 * MIB),
        cost_estimate=cost(2 * seq * HD2 * d, seq * (d + ROWS) * 2),
        name="grad_wo",
    )(sc, o0, o1, *dps)


def gqkv_kernel(sc, h0, h1, h2, h3, p0, p1, s0, s1, gq_ref, gk_ref, gv_ref, fq_ref, fk_ref, fv_ref, acc):
    k = pl.program_id(1)
    c = sc[1]

    @pl.when(k == 0)
    def _():
        acc[ALL] = jnp.zeros_like(acc)

    r = k // 2
    xr = r ^ sc[2]
    for n, ref in enumerate((h0, h1, h2, h3)):

        @pl.when(xr == n)
        def _():
            h = ref[ALL]
            for t, part in enumerate((p0, p1, s0, s1)):
                acc[:, ROWS * t : ROWS * t + ROWS] += dot_tn(h, part[ALL])

    @pl.when(k == pl.num_programs(1) - 1)
    def _():
        for t in range(POOL):
            cc = c if t < 2 else 1 - c
            g = t % 2
            base = ROWS * t
            qc = pl.ds(pl.multiple_of(cc * ROWS + HD2 * g, HD2), HD2)
            kv = pl.ds(pl.multiple_of(cc * HD2 + HD * g, HD), HD)
            vq = acc[:, base : base + HD2].astype(BF)
            vk = acc[:, base + HD2 : base + HD2 + HD].astype(BF)
            vv = acc[:, base + HD2 + HD : base + ROWS].astype(BF)
            for ref, cols, val in ((gq_ref, qc, vq), (fq_ref, qc, vq), (gk_ref, kv, vk), (fk_ref, kv, vk), (gv_ref, kv, vv), (fv_ref, kv, vv)):
                ref[:, cols] = val


def gqkv_call(sc, hids, parts):
    seq = parts[0].shape[0]
    half = hids[0].shape[1] // 2
    mrow = half // 2

    def hspec(n):
        def im(m, k, p):
            return (jnp.where((k // 2) ^ p[2] == n, k % 2, 0), 2 * p[1] + m)

        return pl.BlockSpec((HD2, mrow), im)

    pspec = pl.BlockSpec((HD2, ROWS), lambda m, k, p: (k, 0))
    outs = [CHIP, ROWS, ROWS]
    return pl.pallas_call(
        gqkv_kernel,
        grid_spec=pltpu.PrefetchScalarGridSpec(
            num_scalar_prefetch=1,
            grid=(2, 8),
            in_specs=[hspec(n) for n in range(POOL)] + [pspec] * POOL,
            out_specs=[pl.BlockSpec((mrow, w), lambda m, k, p: (m, 0)) for w in outs]
            + [pl.BlockSpec((mrow, w), lambda m, k, p: (2 * p[1] + m, 0)) for w in outs],
            scratch_shapes=[pltpu.VMEM((mrow, SEQ), F32)],
        ),
        out_shape=[jax.ShapeDtypeStruct((half, w), BF) for w in outs] + [jax.ShapeDtypeStruct((2 * half, w), BF) for w in outs],
        compiler_params=params(2, vmem=54 * MIB),
        cost_estimate=cost(2 * seq * half * SEQ, seq * SEQ * POOL + half * SEQ * 2),
        name="grad_wqkv",
    )(sc, *hids, *parts)


def dhid_kernel(sc, p0, p1, s0, s1, wq, wk, wv, xa, xb, dya, dyb, bs, gain, dm_ref, dx_ref, gp_ref, dq_s, dk_s, dv_s, dh_s):
    i = pid()
    nb = pl.num_programs(0) // 2
    own_chip = (i // nb) == sc[0]
    c = sc[1]
    for t, part in enumerate((p0, p1, s0, s1)):
        cc = c if t < 2 else 1 - c
        g = t % 2
        dq_s[:, pl.ds(pl.multiple_of(cc * ROWS + HD2 * g, HD2), HD2)] = part[:, :HD2]
        kv = pl.ds(pl.multiple_of(cc * HD2 + HD * g, HD), HD)
        dk_s[:, kv] = part[:, HD2:HD3]
        dv_s[:, kv] = part[:, HD3:]
    for n in range(5):
        sl = slice(HD2 * n, HD2 * n + HD2)
        acc = dot_nt(dq_s[ALL], wq[sl, :])
        acc = acc + dot_nt(dk_s[ALL], wk[sl, :])
        acc = acc + dot_nt(dv_s[ALL], wv[sl, :])
        dh_s[:, sl] = acc.astype(BF).astype(F32)
    dh = dh_s[ALL]
    x = jnp.where(own_chip, xa[ALL], xb[ALL]).astype(F32)
    rs = lax.rsqrt(jnp.mean(x * x, axis=1, keepdims=YES) + EPS)
    n = x * rs
    g1 = ONE + gain[ALL]
    dhn = dh * n

    @pl.when(i == 0)
    def _():
        gp_ref[ALL] = jnp.zeros_like(gp_ref)

    gp_ref[ALL] += jnp.sum(dhn, axis=0, keepdims=YES)
    mean = jnp.mean(dhn * g1, axis=1, keepdims=YES)
    dx = ((dh * g1 - n * mean) * rs).astype(BF).astype(F32)
    dy = jnp.where(own_chip, dya[ALL], dyb[ALL]).astype(F32)
    dm = (dy + dx).astype(BF)
    dm_ref[ALL] = dm

    @pl.when(own_chip)
    def _():
        dx_ref[ALL] = jnp.where(bs[ALL] >= 0, jnp.zeros_like(dm), dm)


def dhid_call(sc, parts, wq, wk, wv, x_mine, x_peer, dy_mine, dy_peer, bs_col, gain):
    rows, d = x_mine.shape
    rb = HD
    nb = rows // rb

    def prow(i, s):
        return ((i // nb) * 2 + s[1]) * nb + i % nb

    def own(i, s):
        return (jnp.clip(i - nb * s[0], 0, nb - 1), 0)

    def peer(i, s):
        return (jnp.clip(i - nb * (1 - s[0]), 0, nb - 1), 0)

    pspec = pl.BlockSpec((rb, ROWS), lambda i, s: (prow(i, s), 0))
    return pl.pallas_call(
        dhid_kernel,
        grid_spec=pltpu.PrefetchScalarGridSpec(
            num_scalar_prefetch=1,
            grid=(2 * nb,),
            in_specs=[pspec] * POOL
            + [const_spec(wq.shape), const_spec(wk.shape), const_spec(wv.shape)]
            + [pl.BlockSpec((rb, d), own), pl.BlockSpec((rb, d), peer)] * 2
            + [pl.BlockSpec((rb, 1), lambda i, s: (prow(i, s), 0)), const_spec((1, d))],
            out_specs=[
                pl.BlockSpec((rb, d), lambda i, s: (i, 0)),
                pl.BlockSpec((rb, d), own),
                pl.BlockSpec((1, d), lambda i, s: (0, 0)),
            ],
            scratch_shapes=[
                pltpu.VMEM((rb, CHIP), BF),
                pltpu.VMEM((rb, ROWS), BF),
                pltpu.VMEM((rb, ROWS), BF),
                pltpu.VMEM((rb, d), F32),
            ],
        ),
        out_shape=[
            jax.ShapeDtypeStruct((2 * rows, d), BF),
            jax.ShapeDtypeStruct((rows, d), BF),
            jax.ShapeDtypeStruct((1, d), F32),
        ],
        compiler_params=params(1, vmem=54 * MIB),
        cost_estimate=cost(2 * 2 * rows * d * SEQ, rows * 2 * d * 8 + d * SEQ * 2),
        name="d_hidden",
    )(sc, *parts, wq, wk, wv, x_mine, x_peer, dy_mine, dy_peer, bs_col, gain)


def dsoft_kernel(sc, own_ref, sib_ref, out_ref, buf, sem):
    n = pid()
    c = sc[0]
    last = pl.num_programs(0) - 1

    def copies(im, slot, act):
        for t in range(2):
            b = jnp.minimum(sc[1 + im] + t, 15)
            r = b // POOL
            row = pl.multiple_of(((r // 2) * POOL + b % POOL) * HD, HD)
            dst = buf.at[slot, pl.ds(HD * t, HD), :]
            mine = (r % 2) == c

            @pl.when(mine)
            def _():
                cp = pltpu.make_async_copy(own_ref.at[pl.ds(row, HD), :], dst, sem.at[slot, t])
                cp.start() if act == "start" else cp.wait()

            @pl.when(jnp.logical_not(mine))
            def _():
                cp = pltpu.make_async_copy(sib_ref.at[pl.ds(row, HD), :], dst, sem.at[slot, t])
                cp.start() if act == "start" else cp.wait()

    @pl.when(n == 0)
    def _():
        copies(0, 0, "start")

    @pl.when(n < last)
    def _():
        copies(n + 1, (n + 1) % 2, "start")

    slot = n % 2
    copies(n, slot, "wait")
    off = sc[9 + n]
    row = lax.broadcasted_iota(jnp.int32, (HD, HD2), 0)
    col = lax.broadcasted_iota(jnp.int32, (HD, HD2), 1)
    pick = jnp.where(col == row + off, ONE, 0.0).astype(BF)
    out_ref[ALL] = dot(pick, buf[slot]).astype(BF)


def dsoft_call(sc, dm_own, dm_sib):
    d = dm_own.shape[1]
    return pl.pallas_call(
        dsoft_kernel,
        grid_spec=pltpu.PrefetchScalarGridSpec(
            num_scalar_prefetch=1,
            grid=(8,),
            in_specs=[ANY, ANY],
            out_specs=pl.BlockSpec((HD, d), lambda n, s: (n, 0)),
            scratch_shapes=[pltpu.VMEM((2, HD2, d), BF), pltpu.SemaphoreType.DMA((2, 2))],
        ),
        out_shape=jax.ShapeDtypeStruct((CHIP, d), BF),
        compiler_params=params(1, vmem=24 * MIB),
        cost_estimate=cost(2 * CHIP * HD2 * d, 3 * CHIP * d * 2),
        name="d_soft",
    )(sc, dm_own, dm_sib)


def dvis_kernel(sc, ds_ref, wp, pooled_ref, gain, out_ref, gp_ref, dp_s):
    i = pid()

    @pl.when(i == 0)
    def _():
        dn = dot_nt(ds_ref[ALL], wp[ALL]).astype(BF).astype(F32)
        pv = pooled_ref[ALL].astype(F32)
        rs = lax.rsqrt(jnp.mean(pv * pv, axis=1, keepdims=YES) + EPS)
        n = pv * rs
        g1 = ONE + gain[ALL]
        dnn = dn * n
        gp_ref[ALL] = jnp.sum(dnn, axis=0, keepdims=YES)
        mean = jnp.mean(dnn * g1, axis=1, keepdims=YES)
        dp_s[ALL] = (((dn * g1 - n * mean) * rs).astype(BF).astype(F32) * (ONE / 16.0)).astype(BF)

    row = lax.broadcasted_iota(jnp.int32, (ROWS, GRID), 0)
    tok = lax.broadcasted_iota(jnp.int32, (ROWS, GRID), 1)
    hit = (tok // SIDE == row // HD) & (tok % SIDE == (row % GRID) // POOL)
    mask = jnp.where(hit, ONE, 0.0).astype(BF)
    out_ref[0] = dot(mask, dp_s[pl.ds(pl.multiple_of(i * GRID, GRID), GRID), :]).astype(BF)


def dvis_call(sc, d_soft, wp, pooled, gain):
    n, dv = pooled.shape
    d = d_soft.shape[1]
    return pl.pallas_call(
        dvis_kernel,
        grid_spec=pltpu.PrefetchScalarGridSpec(
            num_scalar_prefetch=1,
            grid=(n // GRID,),
            in_specs=[
                pl.BlockSpec((n, d), lambda i, s: (s[0], 0), pipeline_mode=pl.Buffered(1)),
                const_spec(wp.shape),
                const_spec(pooled.shape),
                const_spec((1, dv)),
            ],
            out_specs=[pl.BlockSpec((1, ROWS, dv), lambda i, s: (i // POOL, i % POOL, 0)), pl.BlockSpec((1, dv), lambda i, s: (0, 0))],
            scratch_shapes=[pltpu.VMEM((n, dv), BF)],
        ),
        out_shape=[jax.ShapeDtypeStruct((n // BLK, GRID * GRID, dv), BF), jax.ShapeDtypeStruct((1, dv), F32)],
        compiler_params=params(1, vmem=24 * MIB),
        cost_estimate=cost(2 * n * d * dv + 2 * n * SIDE * HD * dv, n * SIDE * dv * 2 + wp.size * 2),
        name="d_vis",
    )(sc, d_soft, wp, pooled, gain)


def tail_kernel(sc, normed, ds, sq, sk, sv, go_x, go_s, go_d, fq_in, fk_in, fv_in, fo_in, out_ref, fq, fk, fv, fo, sem):
    i = pid()
    row = pl.multiple_of(sc[0] + i * HD, HD)
    orow = jnp.minimum(i, 3) * LANES
    cps = [pltpu.make_async_copy(src, dst.at[pl.ds(row, HD), :], sem.at[n]) for n, (src, dst) in enumerate(((sq, fq), (sk, fk), (sv, fv)))]
    for n, src in enumerate((go_x, go_s, go_d)):
        at = pl.multiple_of(sc[1 + n] + orow, LANES)
        cps.append(pltpu.make_async_copy(src, fo.at[pl.ds(at, LANES), :], sem.at[3 + n]))
    for cp in cps:
        cp.start()
    out_ref[ALL] = dot_tn(normed[ALL], ds[ALL]).astype(BF)
    for cp in cps:
        cp.wait()


def tail_call(sc, normed, ds, halves, quarters, fulls):
    tok, dv = normed.shape
    d = ds.shape[1]
    half = lambda w: pl.BlockSpec((HD, w), lambda i, s: (i, 0))
    quarter = pl.BlockSpec((LANES, d), lambda i, s: (jnp.minimum(i, 3), 0))
    return pl.pallas_call(
        tail_kernel,
        grid_spec=pltpu.PrefetchScalarGridSpec(
            num_scalar_prefetch=1,
            grid=(5,),
            in_specs=[const_spec(normed.shape), pl.BlockSpec((tok, HD2), lambda i, s: (0, i))]
            + [half(h.shape[1]) for h in halves]
            + [quarter] * 3
            + [ANY] * POOL,
            out_specs=[pl.BlockSpec((dv, HD2), lambda i, s: (0, i))] + [ANY] * POOL,
            scratch_shapes=[pltpu.SemaphoreType.DMA((6,))],
        ),
        out_shape=[jax.ShapeDtypeStruct((dv, d), BF)] + [jax.ShapeDtypeStruct(f.shape, BF) for f in fulls],
        input_output_aliases={9 + n: 1 + n for n in range(POOL)},
        compiler_params=params(1, vmem=32 * MIB),
        cost_estimate=cost(2 * tok * dv * d, tok * (d + dv) * 2 + dv * d * 2),
        name="tail",
    )(sc, normed, ds, *halves, *quarters, *fulls)


def solution(mesh):
    seq_spec = P(('dp', 'cp'))
    part_spec = P('dp')
    rep_spec = P()

    def body(vis, text, img_pos, grad_y, pn_gain, w_proj, pre_gain, w_query, w_key, w_value, q_gain, k_gain, w_out, post_gain):
        rank = lax.axis_index('cp')
        x = rank // 2
        c = rank % 2
        seq = POOL * text.shape[0]
        row_f32 = lambda g: g.astype(F32)[jnp.newaxis, :]
        ints = lambda *v: jnp.stack([jnp.asarray(e, jnp.int32) for e in v])

        pos = img_pos.astype(jnp.int32)
        ids = jnp.arange(8, dtype=jnp.int32)
        start = (jnp.arange(SIDE, dtype=jnp.int32) * HD)[:, jnp.newaxis]
        at_a = (pos[jnp.newaxis] <= start) & (pos[jnp.newaxis] + BLK > start)
        at_b = (pos[jnp.newaxis] > start) & (pos[jnp.newaxis] < start + HD)

        def pick(hit):
            idx = jnp.sum(jnp.where(hit, ids[jnp.newaxis], 0), axis=1)
            shift = jnp.where(jnp.any(hit, axis=1), start[:, 0] - jnp.sum(jnp.where(hit, pos[jnp.newaxis], 0), axis=1), FAR)
            return idx, shift

        ia, da = pick(at_a)
        ib, db = pick(at_b)
        tab = jnp.stack([ia, da, ib, db], axis=1).reshape(-1)
        rows = jnp.arange(seq, dtype=jnp.int32)
        inside = (rows[:, jnp.newaxis] >= pos[jnp.newaxis]) & (rows[:, jnp.newaxis] < pos[jnp.newaxis] + BLK)
        blk_start = jnp.where(jnp.any(inside, axis=1), jnp.sum(jnp.where(inside, pos[jnp.newaxis], 0), axis=1), -FAR)
        bs_col = blk_start[:, jnp.newaxis]
        bs_row = blk_start.reshape(seq // QB, 1, QB)
        qb_lo = jnp.arange(seq // QB, dtype=jnp.int32) * QB
        cross = (pos[jnp.newaxis] < (qb_lo + QB)[:, jnp.newaxis]) & (pos[jnp.newaxis] + BLK > (qb_lo + QB)[:, jnp.newaxis])
        cross = jnp.any(cross, axis=1).astype(jnp.int32)
        nblk = jnp.arange(seq // QB, dtype=jnp.int32)
        nkv = nblk + 1 + cross
        first_q = nblk - jnp.concatenate([jnp.zeros((1,), jnp.int32), cross[:-1]])

        def swap(a, perm):
            return lax.ppermute(a, 'cp', perm)

        pooled, normed = pool_call(vis, row_f32(pn_gain))
        normed_x = swap(normed, XPERM)
        text_x = swap(text, XPERM)
        dy_x = swap(grad_y, XPERM)
        theirs = swap(jnp.stack([normed, normed_x]), SPERM)
        normed_all = jnp.zeros((POOL,) + normed.shape, BF)
        for piece, slot in ((normed, 0), (normed_x, 2), (theirs[0], 1), (theirs[1], 3)):
            normed_all = lax.dynamic_update_index_in_dim(normed_all, piece, rank ^ slot, 0)
        normed_all = normed_all.reshape(-1, normed.shape[1])
        soft = jnp.dot(normed_all, w_proj, preferred_element_type=F32).astype(BF)

        pre = row_f32(pre_gain)
        qg, kg = row_f32(q_gain), row_f32(k_gain)
        x_mine, h_mine = merge_call(tab, ints(rank), soft, text, pre)
        h_sib = swap(h_mine, SPERM)
        inv_freq = ROPE_BASE ** (-jnp.arange(0, HD, 2).astype(F32) / HD)
        angle = (rows.astype(F32) / ROPE_SCALE)[:, jnp.newaxis] * inv_freq[jnp.newaxis, :]
        cos, sin = jnp.cos(angle), jnp.sin(angle)
        qkv_args = (w_query, w_key, w_value, qg, kg, cos, sin)
        bufs = qkv_call(ints(x, c), h_mine, h_sib, *qkv_args, ())
        x_peer, h_peer = merge_call(tab, ints(rank ^ 2), soft, text_x, pre)
        h_diag = swap(h_peer, SPERM)
        q0, q1, qr0, qr1, k0, k1, kr0, kr1, v0, v1 = qkv_call(ints(1 - x, c), h_peer, h_diag, *qkv_args, bufs)

        o0, lse0 = fwd_call(nkv, q0, k0, v0, bs_col)
        o0s = swap(o0, SPERM)
        o1, lse1 = fwd_call(nkv, q1, k1, v1, bs_col)
        o1s = swap(o1, SPERM)

        post = row_f32(post_gain)
        y, dp_m, dam0, dam1, das0, das1, gpost_m = out_call(ints(x, c), (o0, o1), (o0s, o1s), w_out, grad_y, post, (x_mine,))
        das0, das1 = swap(das0, SPERM), swap(das1, SPERM)
        dp_sm = swap(dp_m, SPERM)
        dp_p, dap0, dap1, dbs0, dbs1, gpost_p = out_call(ints(1 - x, c), (o0, o1), (o0s, o1s), w_out, dy_x, post)
        dbs0, dbs1 = swap(dbs0, SPERM), swap(dbs1, SPERM)
        dp_sp = swap(dp_p, SPERM)

        bsc = jnp.concatenate([ints(rank), first_q])
        bwd_args = (cos, sin, qg, kg)
        part0, gq0, gk0 = bwd_call(bsc, q0, (dam0, dap0, das0, dbs0), o0, k0, v0, lse0, bs_row, qr0, kr0, *bwd_args)
        part0s = swap(part0, SPERM)
        part1, gq1, gk1 = bwd_call(bsc, q1, (dam1, dap1, das1, dbs1), o1, k1, v1, lse1, bs_row, qr1, kr1, *bwd_args)
        part1s = swap(part1, SPERM)

        go, go_full = gwo_call(ints(x, c, rank, *[rank ^ n for n in SLOT]), o0, o1, (dp_m, dp_p, dp_sm, dp_sp))
        go_x = swap(go, XPERM)
        go_s = swap(go, SPERM)
        early = jnp.concatenate([gq0 + gq1, gk0 + gk1, gpost_m + gpost_p], axis=1)
        early = early + swap(early, SPERM)

        parts = (part0, part1, part0s, part1s)
        dm, grad_text, gpre = dhid_call(ints(x, c), parts, w_query, w_key, w_value, x_mine, x_peer, grad_y, dy_x, bs_col, pre)
        dm_s = swap(dm, SPERM)
        gpre = gpre + swap(gpre, SPERM)
        go_d = swap(go_x, SPERM)
        *g_half, fq, fk, fv = gqkv_call(ints(x, c, rank), (h_mine, h_sib, h_peer, h_diag), parts)
        halves = [swap(a, SPERM) for a in g_half]
        d_soft = dsoft_call(jnp.concatenate([ints(c), pos // HD, pos % HD]), dm, dm_s)
        grad_vis, gpn = dvis_call(ints(rank), d_soft, w_proj, pooled, row_f32(pn_gain))
        gpn = gpn + swap(gpn, XPERM)
        gpn = gpn + swap(gpn, SPERM)
        where = ints((1 - c) * w_query.shape[0] // 2, (2 * c + 1 - x) * HD2, (2 - 2 * c + x) * HD2, (3 - 2 * c - x) * HD2)
        g_proj, gq, gk, gv, g_out = tail_call(where, normed_all, d_soft, halves, (go_x, go_s, go_d), (fq, fk, fv, go_full))

        early = early[0].astype(BF)
        sq, sk, spost = early[:HD], early[HD:HD2], early[HD2:]
        return (y, grad_text, grad_vis, gpn[0].astype(BF), g_proj, gpre[0].astype(BF), gq, gk, gv, sq, sk, g_out, spost)

    in_specs = (seq_spec, seq_spec, part_spec, seq_spec) + (rep_spec,) * NBUF
    out_specs = (seq_spec, seq_spec, seq_spec) + (part_spec,) * NBUF
    return jax.shard_map(body, mesh=mesh, in_specs=in_specs, out_specs=out_specs, check_vma=False)
```

```python
import functools
import jax
import jax.numpy as jnp
from jax import lax
from jax.experimental import pallas as pl
from jax.experimental.pallas import tpu as pltpu
from jax.sharding import PartitionSpec as P


GRID = 64
POOL = 4
SIDE = GRID // POOL
BLK = SIDE * SIDE
HD = BLK
HALF = HD // 2
HD2 = 2 * HD
HD3 = 3 * HD
ROWS = 4 * HD
CHIP = 2 * ROWS
SEQ = 2 * CHIP
LANES = HALF
YES = True
ALL = ...
NONE = None
ONE = 1.0
EPS = 1e-6
ROPE_BASE = 1000000.0
ROPE_SCALE = 8.0
NEG_BIG = -1e30
LOG2E = 1.4426950408889634
QSCALE = 0.0625
BF = jnp.bfloat16
F32 = jnp.float32
MIB = 1 << 20
FAR = MIB
VMEM_MAX = 67043328 - MIB
SLOT = (0, 2, 1, 3)
XPERM = [(0, 2), (2, 0), (1, 3), (3, 1)]
SPERM = [(0, 1), (1, 0), (2, 3), (3, 2)]
ANY = pl.BlockSpec(memory_space=pl.ANY)
DMA = pltpu.SemaphoreType.DMA


def pid(axis=0):
    return pl.program_id(axis)


def dot(a, b):
    return lax.dot_general(a, b, (((1,), (0,)), ((), ())), preferred_element_type=F32)


def dot_nt(a, b):
    return lax.dot_general(a, b, (((1,), (1,)), ((), ())), preferred_element_type=F32)


def dot_tn(a, b):
    return lax.dot_general(a, b, (((0,), (0,)), ((), ())), preferred_element_type=F32)


def mean1(v):
    return jnp.mean(v, axis=1, keepdims=YES)


def sum1(v):
    return jnp.sum(v, axis=1, keepdims=YES)


def sum0(v):
    return jnp.sum(v, axis=0, keepdims=YES)


def inv_rms(v):
    return lax.rsqrt(mean1(v * v) + EPS)


def iota(dims, axis):
    return lax.broadcasted_iota(jnp.int32, dims, axis)


def at(start, size):
    return pl.ds(pl.multiple_of(start, size), size)


def onehot(hit):
    return jnp.where(hit, ONE, 0.0).astype(BF)


def bcast(v, width=LANES):
    return jnp.broadcast_to(v, (v.shape[0], width))


def whole(dims):
    return pl.BlockSpec(dims, lambda *a: (0,) * len(dims), pipeline_mode=pl.Buffered(1))


def once(dims):
    return pl.BlockSpec(dims, lambda *a: (0,) * len(dims))


def rowspec(rows, width):
    return pl.BlockSpec((rows, width), lambda i, *a: (i, 0))


def launch(kernel, grid, ins, outs, shapes, args, flops, nbytes, prefetch=1, scratch=(), alias=()):
    return pl.pallas_call(
        kernel,
        grid_spec=pltpu.PrefetchScalarGridSpec(
            num_scalar_prefetch=prefetch, grid=grid, in_specs=ins, out_specs=outs, scratch_shapes=scratch
        ),
        out_shape=[jax.ShapeDtypeStruct(dims, BF if len(s) == 0 else s[0]) for dims, *s in shapes],
        input_output_aliases=dict(alias),
        compiler_params=pltpu.CompilerParams(dimension_semantics=("arbitrary",) * len(grid), vmem_limit_bytes=VMEM_MAX),
        cost_estimate=pl.CostEstimate(flops=int(flops), bytes_accessed=int(nbytes), transcendentals=0),
    )(*args)


def pool_kernel(vis_ref, gain_ref, pooled_ref, normed_ref):
    row = iota((GRID, ROWS), 0)
    src = iota((GRID, ROWS), 1)
    hit = (row // SIDE == src // HD) & (row % SIDE == (src % GRID) // POOL)
    pooled = (dot(onehot(hit), vis_ref[0]) * (ONE / SIDE)).astype(BF)
    pooled_ref[ALL] = pooled
    wide = pooled.astype(F32)
    normed_ref[ALL] = (wide * inv_rms(wide) * (ONE + gain_ref[ALL])).astype(BF)


def pool_call(vis, gain):
    n, _, dv = vis.shape
    spec = pl.BlockSpec((1, ROWS, dv), lambda i: (i // POOL, i % POOL, 0))
    dims = (n * BLK, dv)
    return launch(
        pool_kernel, (n * POOL,), [spec, whole((1, dv))], [rowspec(GRID, dv)] * 2, [(dims,)] * 2, (vis, gain),
        2 * n * BLK * ROWS * dv, vis.size * 2, prefetch=0,
    )


def merge_kernel(tab, sc, normed, wp, gain, ta, tb, x_ref, h_ref, n_ref):
    b = sc[0] * POOL + pid()
    ia, da, ib, db = [tab[POOL * b + n] for n in range(POOL)]
    some = (da < FAR) | (db < FAR)
    text = jnp.where(pid() == 0, ta[ALL], tb[ALL])

    @pl.when(some)
    def _():
        row = iota((HD, HD), 0)
        col = iota((HD, HD), 1)
        took = dot(onehot(col == row + da), normed[at(ia * HD, HD), :]) + dot(onehot(col == row + db), normed[at(ib * HD, HD), :])
        took = took.astype(BF)
        n_ref[ALL] = took
        val = dot(took, wp[ALL]).astype(BF)
        r1 = iota((HD, 1), 0)
        ina = (r1 + da >= 0) & (r1 + da < BLK)
        inb = (r1 + db >= 0) & (r1 + db < BLK)
        x_ref[ALL] = jnp.where(ina | inb, val, text)

    @pl.when(jnp.logical_not(some))
    def _():
        n_ref[ALL] = jnp.zeros_like(n_ref)
        x_ref[ALL] = text

    g1 = ONE + gain[ALL]
    for r in range(0, HD, SIDE):
        xv = x_ref[r : r + SIDE, :].astype(F32)
        h_ref[r : r + SIDE, :] = (xv * inv_rms(xv) * g1).astype(BF)


def merge_call(tab, rr, normed, wp, gain, first, rest):
    dv, d = wp.shape
    skip = (ROWS - rest.shape[0]) // HD
    back = pl.BlockSpec((HD, d), lambda i, *a: (jnp.maximum(i - skip, 0), 0))
    spec = rowspec(HD, d)
    return launch(
        merge_kernel, (ROWS // HD,), [whole(normed.shape), whole(wp.shape), whole((1, d)), once((HD, d)), back],
        [spec, spec, rowspec(HD, dv)], [((ROWS, d),), ((ROWS, d),), ((ROWS, dv),)], (tab, rr, normed, wp, gain, first, rest),
        2 * ROWS * dv * (d + HD2), (ROWS * 3 + dv) * d * 2, prefetch=2,
    )


def rope_fwd(raw, gain, cos, sin):
    n = raw * inv_rms(raw) * (ONE + gain)
    a, b = n[:, :HALF], n[:, HALF:]
    return jnp.concatenate([a * cos - b * sin, b * cos + a * sin], axis=1)


def qkv_kernel(sc, ha, hb, wq, wk, wv, qg, kg, cos_ref, sin_ref, *rest):
    q_o, qr_o, k_o, kr_o, v_o = [rest[len(rest) - 2 * n :][:2] for n in range(5, 0, -1)]
    hid = jnp.where(pid() < 2, ha[ALL], hb[ALL])
    cos, sin = cos_ref[ALL], sin_ref[ALL]
    for g in range(2):
        aq = dot(hid, wq[:, HD2 * g : HD2 * g + HD2]).astype(BF)
        qr_o[g][ALL] = aq
        for h in range(2):
            raw = aq[:, HD * h : HD * h + HD].astype(F32)
            q_o[g][:, HD * h : HD * h + HD] = (rope_fwd(raw, qg[ALL], cos, sin) * QSCALE).astype(BF)
        ak = dot(hid, wk[:, HD * g : HD * g + HD]).astype(BF)
        kr_o[g][ALL] = ak
        k_o[g][ALL] = rope_fwd(ak.astype(F32), kg[ALL], cos, sin).astype(BF)
        v_o[g][ALL] = dot(hid, wv[:, HD * g : HD * g + HD]).astype(BF)


def qkv_call(sc, ha, hb, wq, wk, wv, qg, kg, cos, sin, bufs):
    d = ha.shape[1]

    def outrow(i, s):
        return s[0] * POOL + jnp.where(i < 2, s[1] * 2 + i, (1 - s[1]) * 2 + i - 2)

    def ospec(w):
        return pl.BlockSpec((HD2, w), lambda i, s: (outrow(i, s), 0))

    def wspec(w):
        return pl.BlockSpec((d, w), lambda i, s: (0, s[1]), pipeline_mode=pl.Buffered(1))

    widths = [HD2] * POOL + [HD] * 6
    ins = [
        pl.BlockSpec((HD2, d), lambda i, s: (jnp.minimum(i, 1), 0)),
        pl.BlockSpec((HD2, d), lambda i, s: (jnp.maximum(i - 2, 0), 0)),
        wspec(ROWS), wspec(HD2), wspec(HD2), whole((1, HD)), whole((1, HD)), ospec(HALF), ospec(HALF),
    ]
    args = [sc, ha, hb, wq, wk, wv, qg, kg, cos, sin]
    alias = [(len(args) + n, n) for n in range(len(bufs))]
    return launch(
        qkv_kernel, (POOL,), ins + [ANY] * len(bufs), [ospec(w) for w in widths], [((SEQ, w),) for w in widths],
        args + list(bufs), 2 * CHIP * d * CHIP, CHIP * (d + HD3 * POOL) * 2 + d * CHIP * 2, alias=alias,
    )


QB = HD2
KB = HD2
NQ = SEQ // QB


def fwd_kernel(nkv, q_ref, k_ref, v_ref, bs_ref, o_ref, lse_ref, m_s, l_s, acc_s):
    i = pid()
    m_s[ALL] = jnp.full(m_s.shape, NEG_BIG, F32)
    l_s[ALL] = jnp.zeros(l_s.shape, F32)
    acc_s[ALL] = jnp.zeros(acc_s.shape, F32)

    def step(j, nk, r0, masked):
        nr = QB - r0
        rs = slice(r0, QB)
        off = pl.multiple_of(j * KB, KB)
        kb = k_ref[pl.ds(off, nk), :]
        vb = v_ref[pl.ds(off, nk), :]
        if masked:
            qpos = i * QB + r0 + iota((nr, nk), 0)
            kpos = j * KB + iota((nr, nk), 1)
            rel = kpos - bs_ref[rs, :]
            vis = (kpos <= qpos) | ((rel >= 0) & (rel < BLK))
        ss = [dot_nt(q_ref[rs, HD * h : HD * h + HD], kb) for h in range(2)]
        for h in range(2):
            s = jnp.where(vis, ss[h], NEG_BIG) if masked else ss[h]
            parts = [s[:, LANES * t : LANES * t + LANES] for t in range(nk // LANES)]
            mx = bcast(jnp.max(functools.reduce(jnp.maximum, parts), axis=1, keepdims=YES))
            m_old = m_s[h, rs, :]
            m_new = jnp.maximum(m_old, mx)
            alpha = jnp.exp2((m_old - m_new) * LOG2E)
            ps = [jnp.exp2((t - m_new) * LOG2E) for t in parts]
            l_s[h, rs, :] = l_s[h, rs, :] * alpha + functools.reduce(jnp.add, ps)
            m_s[h, rs, :] = m_new
            p = jnp.concatenate([t.astype(BF) for t in ps], axis=1)
            acc_s[h, rs, :] = acc_s[h, rs, :] * jnp.concatenate([alpha, alpha], axis=1) + dot(p, vb)

    lax.fori_loop(0, i, lambda j, c: (step(j, KB, 0, not YES), c)[1], 0)
    step(i, KB, 0, YES)

    @pl.when(nkv[i] > i + 1)
    def _():
        step(i + 1, BLK, QB - BLK, YES)

    for h in range(2):
        l = bcast(sum1(l_s[h]))
        inv = ONE / l
        o_ref[:, HD * h : HD * h + HD] = (acc_s[h] * jnp.concatenate([inv, inv], axis=1)).astype(BF)
        lse_ref[0, h : h + 1, :] = jnp.transpose(m_s[h] * LOG2E + jnp.log2(l))[0:1, :]


def fwd_call(nkv, q, k, v, bs_col):
    lse = pl.BlockSpec((1, 2, QB), lambda i, *a: (i, 0, 0))
    stat = pltpu.VMEM((2, QB, LANES), F32)
    return launch(
        fwd_kernel, (NQ,), [rowspec(QB, HD2), whole((SEQ, HD)), whole((SEQ, HD)), rowspec(QB, 1)],
        [rowspec(QB, HD2), lse], [((SEQ, HD2),), ((NQ, 2, QB), F32)], (nkv, q, k, v, bs_col),
        5 * SEQ * SEQ * HD, SEQ * HD3 * POOL, scratch=[stat, stat, pltpu.VMEM((2, QB, HD), F32)],
    )


def out_kernel(sc, oo0, oo1, os0, os1, wo, dy_ref, gain, *rest):
    x_ref, y_ref = rest[:2] if len(rest) == 9 else (NONE, NONE)
    dp_ref, *da_refs, gp_ref, a_s = rest[-7:]
    own, sib = sc[1] * ROWS, (1 - sc[1]) * ROWS
    cuts = [pl.ds(pl.multiple_of(b + n, HD2), HD2) for b in (own, sib) for n in (0, HD2)]
    a = functools.reduce(jnp.add, [dot(o[ALL], wo[cut, :]) for o, cut in zip((oo0, oo1, os0, os1), cuts)])
    a_s[ALL] = a.astype(BF)
    g1 = ONE + gain[ALL]

    @pl.when(pid() == 0)
    def _():
        gp_ref[ALL] = jnp.zeros_like(gp_ref)

    total = jnp.zeros((8, gain.shape[1]), F32)
    for r in range(0, HD, SIDE):
        rows = slice(r, r + SIDE)
        a = a_s[rows, :].astype(F32)
        rs = inv_rms(a)
        n = a * rs
        if y_ref is not NONE:
            y_ref[rows, :] = (x_ref[rows, :].astype(F32) + n * g1).astype(BF)
        dy = dy_ref[rows, :].astype(F32)
        dyn = dy * n
        total = total + (dyn[:8] + dyn[8:])
        dp_ref[rows, :] = ((dy * g1 - n * mean1(dyn * g1)) * rs).astype(BF)
    gp_ref[ALL] += sum0(total)
    for ref, cut in zip(da_refs, cuts):
        ref[ALL] = dot_nt(dp_ref[ALL], wo[cut, :]).astype(BF)


def out_call(sc, oo, osib, wo, dy, gain, x=()):
    rows, d = dy.shape
    nb = rows // HD
    ospec = pl.BlockSpec((HD, HD2), lambda i, s: ((s[0] * 2 + s[1]) * nb + i, 0))
    wide = [rowspec(HD, d)]
    extra = len(x)
    return launch(
        out_kernel, (nb,), [ospec] * POOL + [whole(wo.shape)] + wide + [whole((1, d))] + wide * extra,
        wide * (1 + extra) + [rowspec(HD, HD2)] * POOL + [once((1, d))],
        [((rows, d),)] * (1 + extra) + [((rows, HD2),)] * POOL + [((1, d), F32)], (sc, *oo, *osib, wo, dy, gain, *x),
        POOL * rows * d * CHIP, rows * d * 10 + wo.size * 2, scratch=[pltpu.VMEM((HD, d), BF)],
    )


def rope_norm_bwd(dy, raw, gain, cos, sin):
    d1, d2 = dy[:, :HALF], dy[:, HALF:]
    dn = jnp.concatenate([d1 * cos + d2 * sin, d2 * cos - d1 * sin], axis=1)
    rs = inv_rms(raw)
    n = raw * rs
    dnn = dn * n
    g1 = ONE + gain
    return ((dn * g1 - n * mean1(dnn * g1)) * rs).astype(BF), sum0(dnn)


def bwd_kernel(
    sc, q_ref, do_a, do_b, do_c, do_d, o_ref, k_ref, v_ref, lse_ref, bs_ref, qr_ref, kr_ref, cos_ref, sin_ref, qg, kg,
    out_ref, gq_ref, gk_ref, do_s, dl_s, dq_s, dk_s, dv_s, sem,
):
    j = pid()

    @pl.when(j == 0)
    def _():
        cps = []
        for n, src in enumerate((do_a, do_b, do_c, do_d)):
            cps.append(pltpu.make_async_copy(src, do_s.at[at((sc[0] ^ SLOT[n]) * ROWS, ROWS), :], sem.at[n]))
        for cp in cps:
            cp.start()
        dq_s[ALL] = jnp.zeros_like(dq_s)
        gq_ref[ALL] = jnp.zeros_like(gq_ref)
        gk_ref[ALL] = jnp.zeros_like(gk_ref)
        for cp in cps:
            cp.wait()

        def delta(i, carry):
            cut = at(i * QB, QB)
            pr = do_s[cut, :].astype(F32) * o_ref[cut, :].astype(F32)
            for h in range(2):
                col = bcast(sum1(pr[:, HD * h : HD * h + HD]))
                dl_s[i, h : h + 1, :] = jnp.transpose(col)[0:1, :]
            return carry

        lax.fori_loop(0, NQ, delta, 0)

    dk_s[ALL] = jnp.zeros_like(dk_s)
    dv_s[ALL] = jnp.zeros_like(dv_s)

    def step(i, r0, nk, masked):
        nr = QB - r0
        rs = slice(r0, QB)
        cut = pl.ds(pl.multiple_of(i * QB + r0, nr), nr)
        kb, vb = k_ref[:nk, :], v_ref[:nk, :]
        if masked:
            kpos = j * KB + iota((nk, nr), 0)
            qpos = i * QB + r0 + iota((nk, nr), 1)
            rel = kpos - bs_ref[i, :, rs]
            vis = (kpos <= qpos) | ((rel >= 0) & (rel < BLK))
        cols = [slice(HD * h, HD * h + HD) for h in range(2)]
        qs = [q_ref[cut, c] for c in cols]
        dos = [do_s[cut, c] for c in cols]
        st = [dot_nt(kb, q) for q in qs]
        dpt = [dot_nt(vb, d) for d in dos]
        for h in range(2):
            pt = jnp.exp2(st[h] * LOG2E - lse_ref[i, h : h + 1, rs])
            if masked:
                pt = jnp.where(vis, pt, 0.0)
            dst = (pt * (dpt[h] - dl_s[i, h : h + 1, rs])).astype(BF)
            dv_s[:nk, :] += dot(pt.astype(BF), dos[h])
            dk_s[:nk, :] += dot(dst, qs[h])
            dq_s[cut, cols[h]] += dot_tn(dst, kb)

    @pl.when(sc[1 + j] < j)
    def _():
        step(jnp.maximum(j - 1, 0), QB - BLK, BLK, YES)

    step(j, 0, KB, YES)
    lax.fori_loop(j + 1, NQ, lambda i, cr: (step(i, 0, KB, not YES), cr)[1], 0)

    cut = at(j * KB, KB)
    dk = dk_s[ALL].astype(BF).astype(F32)
    dk, gk = rope_norm_bwd(dk, kr_ref[ALL].astype(F32), kg[ALL], cos_ref[cut, :], sin_ref[cut, :])
    gk_ref[ALL] += gk
    out_ref[cut, HD2:HD3] = dk
    out_ref[cut, HD3:] = dv_s[ALL].astype(BF)

    @pl.when(j == NQ - 1)
    def _():
        def fin(i, carry):
            cut = at(i * HD, HD)
            cos, sin = cos_ref[cut, :], sin_ref[cut, :]
            for h in range(2):
                sl = slice(HD * h, HD * h + HD)
                dq = (dq_s[cut, sl] * QSCALE).astype(BF).astype(F32)
                dqr, gq = rope_norm_bwd(dq, qr_ref[cut, sl].astype(F32), qg[ALL], cos, sin)
                gq_ref[ALL] += gq
                out_ref[cut, sl] = dqr
            return carry

        lax.fori_loop(0, SEQ // HD, fin, 0)


def bwd_call(sc, q, dos, o, k, v, lse, bs_row, qr, kr, cos, sin, qg, kg):
    full, trig, gain = whole((SEQ, HD2)), whole((SEQ, HALF)), whole((1, HD))
    head = rowspec(KB, HD)
    ins = [full, ANY, ANY, ANY, ANY, full, head, head, whole(lse.shape), whole(bs_row.shape), full, head, trig, trig, gain, gain]
    scratch = [
        pltpu.VMEM((SEQ, HD2), BF), pltpu.VMEM((NQ, 2, QB), F32), pltpu.VMEM((SEQ, HD2), F32),
        pltpu.VMEM((KB, HD), F32), pltpu.VMEM((KB, HD), F32), DMA((POOL,)),
    ]
    return launch(
        bwd_kernel, (NQ,), ins, [once((SEQ, ROWS)), once((1, HD)), once((1, HD))],
        [((SEQ, ROWS),), ((1, HD), F32), ((1, HD), F32)], (sc, q, *dos, o, k, v, lse, bs_row, qr, kr, cos, sin, qg, kg),
        12 * SEQ * SEQ * HD, SEQ * SEQ * 2, scratch=scratch,
    )


def choose(index, refs):
    val = refs[0][ALL]
    for n in range(1, len(refs)):
        val = jnp.where(index == n, refs[n][ALL], val)
    return val


def gwo_kernel(sc, o0, o1, dp0, dp1, dp2, dp3, out_ref, full_ref, acc):
    s = pid()

    @pl.when(s == 0)
    def _():
        acc[ALL] = jnp.zeros_like(acc)

    acc[ALL] += dot_tn(choose(sc[0], (o0, o1)), choose(s // 2, (dp0, dp1, dp2, dp3)))

    @pl.when(s == pl.num_programs(0) - 1)
    def _():
        out_ref[ALL] = acc[ALL].astype(BF)
        full_ref[ALL] = acc[ALL].astype(BF)


def gwo_call(sc, o0, o1, dps):
    d = dps[0].shape[1]
    ospec = pl.BlockSpec((HD2, HD2), lambda s, p: (p[3 + s // 2] * 2 + s % 2, 0))
    dspecs = [pl.BlockSpec((HD2, d), lambda s, p, n=n: (jnp.clip(s - 2 * n, 0, 1), 0)) for n in range(POOL)]
    return launch(
        gwo_kernel, (NQ,), [ospec, ospec] + dspecs,
        [once((HD2, d)), pl.BlockSpec((HD2, d), lambda s, p: (2 * p[1] + p[0], 0))], [((HD2, d),), ((CHIP, d),)],
        (sc, o0, o1, *dps), 2 * SEQ * HD2 * d, SEQ * (d + ROWS) * 2, scratch=[pltpu.VMEM((HD2, d), F32)],
    )


def placed(pieces, sem):
    cps = [
        pltpu.make_async_copy(src, dst.at[pl.ds(pl.multiple_of(row, SIDE), src.shape[0]), cols], sem.at[n])
        for n, (src, dst, row, cols) in enumerate(pieces)
    ]
    for cp in cps:
        cp.start()
    return cps


def gw_body(sc, hids, parts, acc):
    k = pid(1)

    @pl.when(k == 0)
    def _():
        acc[ALL] = jnp.zeros_like(acc)

    h = choose((k // 2) ^ sc[2], hids)
    for t, part in enumerate(parts):
        acc[:, HD2 * t : HD2 * t + HD2] += dot_tn(h, part[ALL])
    return k == pl.num_programs(1) - 1


def gq_kernel(sc, *refs):
    out_ref, full_ref, acc = refs[8:]
    last = gw_body(sc, refs[:4], refs[4:8], acc)

    @pl.when(last)
    def _():
        for t in range(POOL):
            core = sc[1] if t < 2 else 1 - sc[1]
            cols = pl.ds(pl.multiple_of(core * ROWS + HD2 * (t % 2), HD2), HD2)
            val = acc[:, HD2 * t : HD2 * t + HD2].astype(BF)
            out_ref[:, cols] = val
            full_ref[:, cols] = val


def gkv_kernel(sc, *refs):
    outs, acc = refs[8:12], refs[12]
    last = gw_body(sc, refs[:4], refs[4:8], acc)

    @pl.when(last)
    def _():
        for t in range(POOL):
            core = sc[1] if t < 2 else 1 - sc[1]
            cols = pl.ds(pl.multiple_of(core * HD2 + HD * (t % 2), HD), HD)
            for w in range(2):
                val = acc[:, HD2 * t + HD * w : HD2 * t + HD * w + HD].astype(BF)
                outs[w][:, cols] = val
                outs[w + 2][:, cols] = val


def gw_call(sc, hids, parts, both):
    d = hids[0].shape[1]
    tile = d // POOL
    nm = 1 + both

    def hspec(n):
        def im(m, k, p):
            return (jnp.where((k // 2) ^ p[2] == n, k % 2, 0), 2 * p[1] + m if both else p[2])

        return pl.BlockSpec((HD2, tile), im)

    pspec = pl.BlockSpec((HD2, HD2), lambda m, k, p: (k, both))
    width = CHIP // nm
    local = pl.BlockSpec((tile, width), lambda m, k, p: (m, 0))
    put = pl.BlockSpec((tile, width), lambda m, k, p: (2 * p[1] + m if both else p[2], 0))
    return launch(
        gkv_kernel if both else gq_kernel, (nm, NQ),
        [hspec(n) for n in range(POOL)] + [pspec] * POOL, [local] * nm + [put] * nm,
        [((nm * tile, width),)] * nm + [((d, width),)] * nm, (sc, *hids, *parts),
        2 * SEQ * nm * tile * CHIP, (SEQ * CHIP + SEQ * tile) * 2 * nm, scratch=[pltpu.VMEM((tile, CHIP), F32)],
    )


def dhid_kernel(
    sc, p0, p1, s0, s1, wq, wk, wv, gain, bs, xa, xb, dya, dyb, dm_out, dx_out, gp_ref,
    dq_s, dk_s, dv_s, dh_s, x_s, dy_s, dm_s, dx_s, gp_s, in_sem, out_sem,
):
    i = pid()
    last = pl.num_programs(0) - 1
    wide = gain.shape[1] // 2
    g1 = ONE + gain[ALL]

    def owned(b):
        return (b // POOL) == sc[0]

    def loads(b, act):
        slot = b % 2
        for mine, srcs in ((owned(b), (xa, dya)), (jnp.logical_not(owned(b)), (xb, dyb))):

            @pl.when(mine)
            def _():
                for n, (src, dst) in enumerate(zip(srcs, (x_s, dy_s))):
                    cp = pltpu.make_async_copy(src.at[at((b % POOL) * HD, HD), :], dst.at[slot], in_sem.at[slot, n])
                    getattr(cp, act)()

    def stores(b, act):
        slot = b % 2
        cp = pltpu.make_async_copy(dm_s.at[slot], dm_out.at[at(b * HD, HD), :], out_sem.at[slot, 0])
        getattr(cp, act)()

        @pl.when(owned(b))
        def _():
            cp = pltpu.make_async_copy(dx_s.at[slot], dx_out.at[at((b % POOL) * HD, HD), :], out_sem.at[slot, 1])
            getattr(cp, act)()

    def norm_bwd(b, n):
        slot = b % 2
        grow = ((b // POOL) * 2 + sc[1]) * ROWS + (b % POOL) * HD
        total = jnp.zeros((8, gain.shape[1]), F32)
        for t in range(HALF // SIDE):
            row = n * HALF + t * SIDE
            rows = at(row, SIDE)
            dh = dh_s[slot, rows, :].astype(F32)
            x = x_s[slot, rows, :].astype(F32)
            rs = inv_rms(x)
            xn = x * rs
            dhn = dh * xn
            total = total + (dhn[:8] + dhn[8:])
            dx = ((dh * g1 - xn * mean1(dhn * g1)) * rs).astype(BF).astype(F32)
            dm = (dy_s[slot, rows, :].astype(F32) + dx).astype(BF)
            dm_s[slot, rows, :] = dm
            text = bs[at(grow + row, SIDE), :] < 0
            dx_s[slot, rows, :] = jnp.where(text, dm, jnp.zeros_like(dm))
        gp_s[ALL] += total

    for t, part in enumerate((p0, p1, s0, s1)):
        core = sc[1] if t < 2 else 1 - sc[1]
        dq_s[:, pl.ds(pl.multiple_of(core * ROWS + HD2 * (t % 2), HD2), HD2)] = part[:, :HD2]
        kv = pl.ds(pl.multiple_of(core * HD2 + HD * (t % 2), HD), HD)
        dk_s[:, kv] = part[:, HD2:HD3]
        dv_s[:, kv] = part[:, HD3:]

    @pl.when(i < 2)
    def _():
        gp_s[ALL] = jnp.zeros_like(gp_s)

    @pl.when(i > 0)
    def _():
        loads(i - 1, "wait")

    loads(i, "start")

    @pl.when(i > 2)
    def _():
        stores(i - 3, "wait")

    def both(n, carry):
        norm_bwd(jnp.maximum(i - 1, 0), n)
        sl = at(n * wide, wide)
        acc = dot_nt(dq_s[ALL], wq[sl, :]) + dot_nt(dk_s[ALL], wk[sl, :]) + dot_nt(dv_s[ALL], wv[sl, :])
        dh_s[i % 2, :, sl] = acc.astype(BF)
        return carry

    lax.fori_loop(0, 2, both, 0)

    @pl.when(i > 0)
    def _():
        stores(i - 1, "start")

    @pl.when(i == last)
    def _():
        loads(last, "wait")
        stores(last - 2, "wait")
        lax.fori_loop(0, 2, lambda n, cr: (norm_bwd(last, n), cr)[1], 0)
        gp_ref[ALL] = sum0(gp_s[ALL])
        stores(last, "start")
        stores(last - 1, "wait")
        stores(last, "wait")


def dhid_call(sc, parts, wq, wk, wv, x_mine, x_peer, dy_mine, dy_peer, bs_col, gain):
    rows, d = x_mine.shape
    nb = rows // HD
    pspec = pl.BlockSpec((HD, ROWS), lambda i, s: (((i // nb) * 2 + s[1]) * nb + i % nb, 0))
    slots = pltpu.VMEM((2, HD, d), BF)
    scratch = [pltpu.VMEM((HD, CHIP), BF), pltpu.VMEM((HD, ROWS), BF), pltpu.VMEM((HD, ROWS), BF)]
    scratch += [slots] * 5 + [pltpu.VMEM((8, d), F32), DMA((2, 2)), DMA((2, 2))]
    return launch(
        dhid_kernel, (2 * nb,),
        [pspec] * POOL + [whole(w.shape) for w in (wq, wk, wv)] + [whole((1, d)), whole(bs_col.shape)] + [ANY] * POOL,
        [ANY, ANY, once((1, d))], [((2 * rows, d),), ((rows, d),), ((1, d), F32)],
        (sc, *parts, wq, wk, wv, gain, bs_col, x_mine, x_peer, dy_mine, dy_peer),
        2 * 2 * rows * d * SEQ, rows * 2 * d * 8 + d * SEQ * 2, scratch=scratch,
    )


def gwp_kernel(
    sc, n0, n1, n2, n3, dm_o, dm_s, wp, pooled, gain, gq_x, gq_s, go_x, go_s, go_d, own_ref, sib_ref, *rest,
):
    half_ref, full_ref, dp_ref, gp_ref, fq, fo, acc, buf, sem, gsem = rest[2:]
    i = pid()
    used = sc[3 + i] > 0
    place = 3 + NQ + POOL
    jobs = zip((gq_x, gq_s, go_x, go_s, go_d), (fq, fq, fo, fo, fo))
    cps = placed([(src, dst, sc[place + n] + i * src.shape[0], slice(NONE)) for n, (src, dst) in enumerate(jobs)], sem)

    def rows_of_image(im, act):
        for t in range(2):
            b = jnp.minimum(sc[3 + NQ + 2 * im] + t, SEQ // HD - 1)
            r = b // POOL
            row = ((r // 2) * POOL + b % POOL) * HD
            for mine, src in (((r % 2) == sc[1], own_ref), ((r % 2) != sc[1], sib_ref)):

                @pl.when(mine)
                def _():
                    cp = pltpu.make_async_copy(src.at[at(row, HD), :], buf.at[im, pl.ds(HD * t, HD), :], gsem.at[im, t])
                    getattr(cp, act)()

    @pl.when(i == 0)
    def _():
        acc[ALL] = jnp.zeros_like(acc)
        for act in ("start", "wait"):
            for im in range(2):
                rows_of_image(im, act)
        row = iota((HD, HD2), 0)
        col = iota((HD, HD2), 1)
        g1 = ONE + gain[ALL]
        total = jnp.zeros_like(gain)
        for im in range(2):
            took = dot(onehot(col == row + sc[3 + NQ + 2 * im + 1]), buf[im]).astype(BF)
            cut = slice(HD * im, HD * im + HD)
            dn = dot_nt(took, wp[ALL]).astype(BF).astype(F32)
            pv = pooled[cut, :].astype(F32)
            rs = inv_rms(pv)
            n = pv * rs
            dnn = dn * n
            total = total + sum0(dnn)
            dp = ((dn * g1 - n * mean1(dnn * g1)) * rs).astype(BF).astype(F32)
            dp_ref[cut, :] = (dp * (ONE / SIDE)).astype(BF)
        gp_ref[ALL] = total

    @pl.when(used)
    def _():
        r = i // 2
        nrow = choose(r ^ sc[2], (n0, n1, n2, n3))
        acc[ALL] += dot_tn(nrow, jnp.where((r % 2) == sc[1], dm_o[ALL], dm_s[ALL]))

    @pl.when(i == pl.num_programs(0) - 1)
    def _():
        half_ref[ALL] = acc[ALL].astype(BF)
        full_ref[ALL] = acc[ALL].astype(BF)

    for cp in cps:
        cp.wait()


def gwp_call(sc, nrows, dm_own, dm_sib, wp, pooled, gain, pieces, fulls):
    dv, d = wp.shape
    cols = d // 2

    def nspec(n):
        return pl.BlockSpec((HD2, dv), lambda i, p: (jnp.where((i // 2) ^ p[2] == n, i % 2, 0), 0))

    dspec = pl.BlockSpec((HD2, cols), lambda i, p: ((i // POOL) * 2 + i % 2, p[1]))
    piece = lambda a: rowspec(a.shape[0] // NQ, a.shape[1])
    args = (sc, *nrows, dm_own, dm_sib, wp, pooled, gain, *pieces, dm_own, dm_sib, *fulls)
    n_in = len(args)
    ins = [nspec(n) for n in range(POOL)] + [dspec] * 2 + [whole(wp.shape), whole(pooled.shape), whole((1, dv))]
    ins += [piece(a) for a in pieces] + [ANY] * (2 + len(fulls))
    return launch(
        gwp_kernel, (NQ,), ins,
        [once((dv, cols)), pl.BlockSpec((dv, cols), lambda i, p: (0, p[1])), once(pooled.shape), once((1, dv))] + [ANY] * len(fulls),
        [((dv, cols),), ((dv, d),), (pooled.shape,), ((1, dv), F32)] + [(f.shape,) for f in fulls], args,
        SEQ * dv * d, SEQ * d * 2, alias=[(n_in - len(fulls) + n, POOL + n) for n in range(len(fulls))],
        scratch=[pltpu.VMEM((dv, cols), F32), pltpu.VMEM((2, HD2, d), BF), DMA((5,)), DMA((2, 2))],
    )


def dvis_kernel(sc, dp_ref, gp_s, gk_s, gv_s, gq_d, *rest):
    out_ref, fp, fk, fv, fq, sem = rest[-6:]
    i = pid()
    cols = pl.ds(pl.multiple_of(sc[0], LANES), gp_s.shape[1])
    cps = placed([(gp_s, fp, i * gp_s.shape[0], cols)], sem.at[pl.ds(0, 1)])
    jobs = ((gk_s, fk, sc[1]), (gv_s, fv, sc[1]), (gq_d, fq, sc[2]))
    cps += placed([(src, dst, row + i * src.shape[0], slice(NONE)) for src, dst, row in jobs], sem.at[pl.ds(1, 3)])
    row = iota((ROWS, GRID), 0)
    tok = iota((ROWS, GRID), 1)
    hit = (tok // SIDE == row // HD) & (tok % SIDE == (row % GRID) // POOL)
    out_ref[0] = dot(onehot(hit), dp_ref[ALL]).astype(BF)
    for cp in cps:
        cp.wait()


def dvis_call(sc, dp, pieces, fulls):
    n, dv = dp.shape
    spec = pl.BlockSpec((1, ROWS, dv), lambda i, s: (i // POOL, i % POOL, 0))
    ins = [rowspec(GRID, dv)] + [rowspec(a.shape[0] // NQ, a.shape[1]) for a in pieces] + [ANY] * POOL
    return launch(
        dvis_kernel, (NQ,), ins, [spec] + [ANY] * POOL,
        [((n // BLK, GRID * GRID, dv),)] + [(f.shape,) for f in fulls], (sc, dp, *pieces, *fulls),
        2 * n * SIDE * HD * dv, n * SIDE * dv * 2, alias=[(6 + n, 1 + n) for n in range(POOL)], scratch=[DMA((POOL,))],
    )


def solution(mesh):
    seq_spec = P(('dp', 'cp'))
    part_spec = P('dp')
    rep_spec = P()

    def body(vis, text, img_pos, grad_y, pn_gain, w_proj, pre_gain, w_query, w_key, w_value, q_gain, k_gain, w_out, post_gain):
        rank = lax.axis_index('cp')
        x = rank // 2
        c = rank % 2
        row_f32 = lambda g: g.astype(F32)[jnp.newaxis, :]
        ints = lambda *v: jnp.stack([jnp.asarray(e, jnp.int32) for e in v])

        def swap(a, perm):
            return lax.ppermute(a, 'cp', perm)

        pos = img_pos.astype(jnp.int32)
        here = pos[jnp.newaxis]
        ids = jnp.arange(pos.shape[0], dtype=jnp.int32)[jnp.newaxis]
        start = (jnp.arange(SEQ // HD, dtype=jnp.int32) * HD)[:, jnp.newaxis]

        def pick(hit):
            idx = jnp.sum(jnp.where(hit, ids, 0), axis=1)
            shift = jnp.where(jnp.any(hit, axis=1), start[:, 0] - jnp.sum(jnp.where(hit, here, 0), axis=1), FAR)
            return idx, shift

        ia, da = pick((here <= start) & (here + BLK > start))
        ib, db = pick((here > start) & (here < start + HD))
        tab = jnp.stack([ia, da, ib, db], axis=1).reshape(-1)
        used = jnp.minimum(da, db).reshape(NQ, -1).min(axis=1) < FAR
        rows = jnp.arange(SEQ, dtype=jnp.int32)
        inside = (rows[:, jnp.newaxis] >= here) & (rows[:, jnp.newaxis] < here + BLK)
        blk_start = jnp.where(jnp.any(inside, axis=1), jnp.sum(jnp.where(inside, here, 0), axis=1), -FAR)
        bs_col = blk_start[:, jnp.newaxis]
        bs_row = blk_start.reshape(NQ, 1, QB)
        nblk = jnp.arange(NQ, dtype=jnp.int32)
        edge = ((nblk + 1) * QB)[:, jnp.newaxis]
        cross = jnp.any((here < edge) & (here + BLK > edge), axis=1).astype(jnp.int32)
        nkv = nblk + 1 + cross
        first_q = nblk - jnp.concatenate([jnp.zeros((1,), jnp.int32), cross[:-1]])

        head_x = swap(text[:HD], XPERM)
        pooled, normed = pool_call(vis, row_f32(pn_gain))
        normed_x = swap(normed, XPERM)
        rest_x = swap(text[HD:], XPERM)
        dy_x = swap(grad_y, XPERM)
        theirs = swap(jnp.stack([normed, normed_x]), SPERM)
        normed_all = jnp.zeros((POOL,) + normed.shape, BF)
        for piece, slot in ((normed, 0), (normed_x, 2), (theirs[0], 1), (theirs[1], 3)):
            normed_all = lax.dynamic_update_index_in_dim(normed_all, piece, rank ^ slot, 0)
        normed_all = normed_all.reshape(-1, normed.shape[1])

        pre = row_f32(pre_gain)
        qg, kg = row_f32(q_gain), row_f32(k_gain)
        x_mine, h_mine, n_mine = merge_call(tab, ints(rank), normed_all, w_proj, pre, text, text)
        h_sib = swap(h_mine, SPERM)
        inv_freq = ROPE_BASE ** (-jnp.arange(0, HD, 2).astype(F32) / HD)
        angle = (rows.astype(F32) / ROPE_SCALE)[:, jnp.newaxis] * inv_freq[jnp.newaxis, :]
        cos, sin = jnp.cos(angle), jnp.sin(angle)
        qkv_args = (w_query, w_key, w_value, qg, kg, cos, sin)
        bufs = qkv_call(ints(x, c), h_mine, h_sib, *qkv_args, ())
        x_peer, h_peer, n_peer = merge_call(tab, ints(rank ^ 2), normed_all, w_proj, pre, head_x, rest_x)
        h_diag = swap(h_peer, SPERM)
        n_sib = swap(n_mine, SPERM)
        n_diag = swap(n_peer, SPERM)
        q0, q1, qr0, qr1, k0, k1, kr0, kr1, v0, v1 = qkv_call(ints(1 - x, c), h_peer, h_diag, *qkv_args, bufs)

        o0, lse0 = fwd_call(nkv, q0, k0, v0, bs_col)
        o0s = swap(o0, SPERM)
        o1, lse1 = fwd_call(nkv, q1, k1, v1, bs_col)
        o1s = swap(o1, SPERM)

        post = row_f32(post_gain)
        y, dp_m, dam0, dam1, das0, das1, gpost_m = out_call(ints(x, c), (o0, o1), (o0s, o1s), w_out, grad_y, post, (x_mine,))
        das0, das1 = swap(das0, SPERM), swap(das1, SPERM)
        dp_sm = swap(dp_m, SPERM)
        dp_p, dap0, dap1, dbs0, dbs1, gpost_p = out_call(ints(1 - x, c), (o0, o1), (o0s, o1s), w_out, dy_x, post)
        dbs0, dbs1 = swap(dbs0, SPERM), swap(dbs1, SPERM)
        dp_sp = swap(dp_p, SPERM)

        bsc = jnp.concatenate([ints(rank), first_q])
        bwd_args = (cos, sin, qg, kg)
        part0, gq0, gk0 = bwd_call(bsc, q0, (dam0, dap0, das0, dbs0), o0, k0, v0, lse0, bs_row, qr0, kr0, *bwd_args)
        part0s = swap(part0, SPERM)
        part1, gq1, gk1 = bwd_call(bsc, q1, (dam1, dap1, das1, dbs1), o1, k1, v1, lse1, bs_row, qr1, kr1, *bwd_args)
        part1s = swap(part1, SPERM)
        early = jnp.concatenate([gq0 + gq1, gk0 + gk1, gpost_m + gpost_p], axis=1)
        early = early + swap(early, SPERM)

        go, go_full = gwo_call(ints(x, c, rank, *[rank ^ n for n in SLOT]), o0, o1, (dp_m, dp_p, dp_sm, dp_sp))
        go_x = swap(go, XPERM)
        go_s = swap(go, SPERM)
        parts = (part0, part1, part0s, part1s)
        hids = (h_mine, h_sib, h_peer, h_diag)
        gq, gq_full = gw_call(ints(x, c, rank), hids, parts, 0)
        gq_x = swap(gq, XPERM)
        gq_s = swap(gq, SPERM)
        dm, grad_text, gpre = dhid_call(ints(x, c), parts, w_query, w_key, w_value, x_mine, x_peer, grad_y, dy_x, bs_col, pre)
        dm_s = swap(dm, SPERM)
        go_d = swap(go_x, SPERM)
        gpre = gpre + swap(gpre, SPERM)
        gk, gv, gk_full, gv_full = gw_call(ints(x, c, rank), hids, parts, 1)
        gq_d = swap(gq_x, SPERM)
        gk_s, gv_s = swap(gk, SPERM), swap(gv, SPERM)
        mine = lax.dynamic_slice_in_dim(pos, 2 * rank, 2)
        quarter = w_query.shape[0] // POOL
        spots = [(rank ^ n) * quarter for n in (2, 1)] + [(2 * c + 1 - x) * HD2, (2 - 2 * c + x) * HD2, (3 - 2 * c - x) * HD2]
        psc = jnp.concatenate([ints(x, c, rank), used.astype(jnp.int32), jnp.stack([mine // HD, mine % HD], axis=1).reshape(-1), ints(*spots)])
        gp, gp_full, dpool, gpn, gq_full, g_out = gwp_call(
            psc, (n_mine, n_sib, n_peer, n_diag), dm, dm_s, w_proj, pooled, row_f32(pn_gain), (gq_x, gq_s, go_x, go_s, go_d),
            (gq_full, go_full),
        )
        gp_s = swap(gp, SPERM)
        gpn = gpn + swap(gpn, XPERM)
        gpn = gpn + swap(gpn, SPERM)
        spots = ints((1 - c) * gp.shape[1], (1 - c) * 2 * quarter, (rank ^ 3) * quarter)
        grad_vis, g_proj, gk, gv, gq = dvis_call(spots, dpool, (gp_s, gk_s, gv_s, gq_d), (gp_full, gk_full, gv_full, gq_full))

        early = early[0].astype(BF)
        sq, sk, spost = early[:HD], early[HD:HD2], early[HD2:]
        return (y, grad_text, grad_vis, gpn[0].astype(BF), g_proj, gpre[0].astype(BF), gq, gk, gv, sq, sk, g_out, spost)

    in_specs = (seq_spec, seq_spec, part_spec, seq_spec) + (rep_spec,) * 10
    out_specs = (seq_spec, seq_spec, seq_spec) + (part_spec,) * 10
    return jax.shard_map(body, mesh=mesh, in_specs=in_specs, out_specs=out_specs, check_vma=not YES)
```
